32 devices in a mesh: gx: 4 (over y, core), gy: 8 (over z, x).
Axes of the slice: x: 2, y: 2, z: 4, core: 2. Of those that a mesh axis runs over, the one named last changes fastest.
Arguments:
- child_value: bfloat16 [524288, 128], P(('gx', 'gy')), may hold values from -6 to 6
- child_row: int32 [32, 16384], P(('gx', 'gy')), may hold values from 0 to 16383, each once within a row
- opp_set: int32 [524288], P(('gx', 'gy')), may hold values from 0 to 65535, as said below
- opp_home: int32 [65536], replicated, may hold values from 0 to 65535, as said below
- opp_cum: float32 [65536, 128], P(('gx', 'gy')), may hold values from 0.01 to 1
- reach: float32 [4096], P(('gx', 'gy')), may hold values from 0.05 to 1
- br_set: int32 [4096], P(('gx', 'gy')), may hold values from 0 to 2047, as said below
- br_home: int32 [2048], replicated, may hold values from 0 to 2047, as said below
- br_cum: float32 [2048, 128], P(('gx', 'gy')), may hold values from 0.01 to 1
Outputs:
- history_value: float32 [524288], P(('gx', 'gy'))
- regret_gap: float32 [2048], P(('gx', 'gy'))
- exploitability: float32 [], replicated
The draws below stay inside these ranges and needn't reach their ends.
Inputs may be any that keep to these rules, and one draw needn't show every extreme that they name: A permutation: opponent infoset i lives in row opp_home[i], owned by device opp_home[i] // 2048. `opp_set`: among the 16384 rows of one device at most 1024 have infosets owned by any one device; in every draw some owner has exactly 1024 from every device. A permutation: best-responder infoset i lives in row br_home[i], owned by device br_home[i] // 64. `br_set`: among the 128 rows of one device at most 8 have infosets owned by any one device; in every draw some owner has exactly 8 from every device.
All inputs are finite; a program needn't handle non-finite values.
Results may differ from the reference program's by a relative error of at most 0.0029.
Values may be sent and summed in bfloat16 or wider, within the bound.
No kernel may reach another device: no remote copies, remote signals or barrier semaphores. Data moves between devices by JAX's collectives and lax.ppermute only.
A program may use at most 128 MiB of HBM per device.

```python
import math
import jax
import jax.numpy as jnp
from jax import lax

ACTIONS = 128
PAR_DEV = 128
S1_DEV = 2048
S2_DEV = 64
DEV_ALL = 32
HIST_DEV = 16384
HIST = 524288
PARENTS = 4096
OPP_SETS = 65536
BR_SETS = 2048
CAP = 1024
CAP2 = 8


def owner_table(key, count, salt):
    return jax.random.permutation(jax.random.fold_in(key, salt), count).astype(jnp.int32)


def pick_sets(key, home, per_owner, rows, limit, devices, salt):
    inverse = jnp.zeros_like(home).at[home].set(jnp.arange(home.shape[0], dtype=jnp.int32))
    favored = jax.random.randint(jax.random.fold_in(key, salt), (), 0, devices)

    def one_device(index):
        sub = jax.random.fold_in(jax.random.fold_in(key, salt + 1), index)
        scores = jax.random.permutation(sub, devices * limit).astype(jnp.int32)
        slots = jnp.arange(devices * limit, dtype=jnp.int32)
        scores = jnp.where(slots // limit == favored, scores - devices * limit, scores)
        order = jnp.argsort(scores, stable=True)[:rows]
        order = order[jax.random.permutation(jax.random.fold_in(sub, 5), rows)]
        owners = (order // limit).astype(jnp.int32)
        local = jax.random.randint(jax.random.fold_in(sub, 7), (rows,), 0, per_owner)
        return inverse[owners * per_owner + local]
    return jax.vmap(one_device)(jnp.arange(devices, dtype=jnp.int32)).reshape(-1)


def draw_opp_home(key, part):
    return owner_table(key, OPP_SETS, 101)


def draw_opp_set(key, part):
    home = owner_table(key, OPP_SETS, 101)
    return pick_sets(key, home, S1_DEV, HIST_DEV, CAP, DEV_ALL, 211)


def draw_br_home(key, part):
    return owner_table(key, BR_SETS, 307)


def draw_br_set(key, part):
    home = owner_table(key, BR_SETS, 307)
    return pick_sets(key, home, S2_DEV, PAR_DEV, CAP2, DEV_ALL, 409)


def level_of(stream_key, extent, pieces, smallest, high):
    level = 1.0
    for axis_at, shards_of in pieces:
        draws = jax.random.uniform(jax.random.fold_in(jax.random.fold_in(stream_key, 6), axis_at), (shards_of,), jnp.float32, smallest / len(pieces), high / len(pieces))
        level = level * jnp.repeat(jnp.exp(draws), extent[axis_at] // shards_of).reshape((-1,) + (1,) * (len(extent) - 1 - axis_at))
    return level


def scatter_about(rng, dims, scale, most, split=(), kind=jnp.bfloat16):
    gain = level_of(rng, dims, split, -0.22, 0.18) if split else 1.0
    result = jax.random.normal(rng, dims, jnp.float32) * scale * gain
    return jnp.minimum(jnp.maximum(result, -most), most).astype(kind)


def setup_inputs(seed: int = 0) -> dict:
    seeds = jax.random.split(jax.random.key(seed), 10)
    return {
        "child_value": scatter_about(seeds[0], (HIST, ACTIONS), 1.0, 6.0, ((0, 32),)),
        "child_row": jax.vmap(lambda own: jax.random.permutation(own, HIST_DEV))(jax.random.split(seeds[1], DEV_ALL)).reshape((DEV_ALL, HIST_DEV)).astype(jnp.int32),
        "opp_set": draw_opp_set(jax.random.fold_in(seeds[9], 71), 0),
        "opp_home": draw_opp_home(jax.random.fold_in(seeds[9], 71), 0),
        "opp_cum": jnp.clip(jnp.exp(math.log(1.0) - 4.6051702 * jax.random.uniform(seeds[4], (OPP_SETS, ACTIONS), jnp.float32) ** level_of(seeds[4], (OPP_SETS, ACTIONS), ((0, 32),), -0.2, 0.2)), 0.01, 1.0),
        "reach": jnp.clip(jnp.exp(math.log(1.0) - 2.9957323 * jax.random.uniform(seeds[5], (PARENTS,), jnp.float32) ** level_of(seeds[5], (PARENTS,), ((0, 32),), -0.2, 0.2)), 0.05, 1.0),
        "br_set": draw_br_set(jax.random.fold_in(seeds[9], 71), 0),
        "br_home": draw_br_home(jax.random.fold_in(seeds[9], 71), 0),
        "br_cum": jnp.clip(jnp.exp(math.log(1.0) - 4.6051702 * jax.random.uniform(seeds[8], (BR_SETS, ACTIONS), jnp.float32) ** level_of(seeds[8], (BR_SETS, ACTIONS), ((0, 32),), -0.2, 0.2)), 0.01, 1.0),
    }


def reference(child_value, child_row, opp_set, opp_home, opp_cum, reach, br_set, br_home, br_cum):
    policy = (opp_cum / jnp.sum(opp_cum, axis=1, keepdims=True)).astype(jnp.bfloat16)
    values = child_value.reshape(DEV_ALL, HIST_DEV, ACTIONS)
    sets = opp_set.reshape(DEV_ALL, HIST_DEV)

    def one_device(item):
        vals, ids, order = item
        rows = policy[opp_home[ids]]
        expect = jnp.sum(rows.astype(jnp.float32) * vals.astype(jnp.float32), axis=1)
        return expect, expect[order]

    expect, chosen = lax.map(one_device, (values, sets, child_row))
    history_value = expect.reshape(HIST)
    weighted = reach[:, None] * chosen.reshape(PARENTS, ACTIONS)
    action_value = jnp.zeros((BR_SETS, ACTIONS), jnp.float32).at[br_home[br_set]].add(weighted)
    br_policy = br_cum / jnp.sum(br_cum, axis=1, keepdims=True)
    regret_gap = jnp.max(action_value, axis=1) - jnp.sum(br_policy * action_value, axis=1)
    exploitability = jnp.sum(regret_gap) / jnp.sum(reach)
    return history_value, regret_gap, exploitability
```

```python
import functools

import jax
import jax.numpy as jnp
from jax import lax
from jax.experimental import pallas as pl
from jax.experimental.pallas import tpu as pltpu
from jax.sharding import PartitionSpec as P


AXES = ("gx", "gy")
LANES = 128
SCALE_BITS = 17
TABLE_LIMIT = 24 * 2**20


def one_hot(hit):
    return jnp.where(hit, 1.0, 0.0).astype(jnp.bfloat16)


def iota(shape, dim):
    return lax.broadcasted_iota(jnp.int32, shape, dim)


def lookup_body(planes_ref, query_ref, out_ref):
    count, high = planes_ref.shape[0] // LANES, planes_ref.shape[1]
    row_of = iota((high, LANES), 0)
    lane_of = iota((LANES, LANES), 0)

    def step(i, carry):
        query = query_ref[pl.ds(i, 1), :]
        rows = one_hot(row_of == (query >> 7))
        picked = jnp.dot(planes_ref[...], rows, preferred_element_type=jnp.float32)
        hit = lane_of == (query & (LANES - 1))
        total = picked[:LANES]
        for k in range(1, count):
            total = total + picked[k * LANES : (k + 1) * LANES] * float(256**k)
        value = jnp.sum(jnp.where(hit, total, 0.0), axis=0, keepdims=True)
        out_ref[pl.ds(i, 1), :] = value.astype(jnp.int32)
        return carry

    lax.fori_loop(0, query_ref.shape[0], step, 0, unroll=2)


def lookup(table, query):
    size = table.shape[0]
    count = max(1, ((size - 1).bit_length() + 7) // 8)
    grid = table.reshape(size // LANES, LANES).T
    planes = jnp.concatenate([(grid >> (8 * k)) & 255 for k in range(count)], axis=0)
    return pl.pallas_call(
        lookup_body,
        out_shape=jax.ShapeDtypeStruct(query.shape, jnp.int32),
        name="lookup",
    )(planes.astype(jnp.float32).astype(jnp.bfloat16), query)


def value_body(blocks, place_ref, odd_ref, child_ref, *rest):
    block_refs, (out_ref, table, sems) = rest[:blocks], rest[blocks:]
    size = block_refs[0].shape[0]
    copies = [
        pltpu.make_async_copy(ref, table.at[pl.ds(8 + b * size, size), :], sems.at[b])
        for b, ref in enumerate(block_refs)
    ]
    for copy in copies:
        copy.start()
    for copy in copies:
        copy.wait()
    sub = iota((8, LANES), 0)
    spot = iota((8, LANES), 1) - sub

    def tile(t, carry):
        low = jnp.zeros((8, LANES), jnp.float32)
        high = jnp.zeros((8, LANES), jnp.float32)
        for g in range(LANES // 16):
            first = pl.multiple_of(t * LANES, LANES) + 16 * g
            child = child_ref[pl.ds(first, 16), :].astype(jnp.float32)
            for half in range(2):
                at = first + 8 * half
                words = table[pl.ds(place_ref[at] + 8, 8), :]
                for s in range(1, 8):
                    row = table[pl.ds(place_ref[at + s] + (8 - s), 8), :]
                    words = jnp.where(sub == s, row, words)
                part = child[8 * half : 8 * half + 8]
                even = (words & 0xFFFF).astype(jnp.float32) * part
                odd = lax.shift_right_logical(words, 16).astype(jnp.float32) * part
                here = spot == 16 * g + 8 * half
                low = jnp.where(here, jnp.sum(even, axis=1, keepdims=True), low)
                high = jnp.where(here, jnp.sum(odd, axis=1, keepdims=True), high)
        low = jnp.sum(low, axis=0, keepdims=True)
        high = jnp.sum(high, axis=0, keepdims=True)
        picked = jnp.where(odd_ref[pl.ds(t, 1), :] > 0, high, low)
        out_ref[pl.ds(t, 1), :] = picked * (0.5**SCALE_BITS)
        return carry

    lax.fori_loop(0, out_ref.shape[0], tile, 0)


def values_from(blocks, place, odd, child_value):
    size = blocks[0].shape[0]
    vmem, smem, hbm = (
        pl.BlockSpec(memory_space=s) for s in (pltpu.VMEM, pltpu.SMEM, pl.ANY)
    )
    return pl.pallas_call(
        functools.partial(value_body, len(blocks)),
        out_shape=jax.ShapeDtypeStruct(odd.shape, jnp.float32),
        in_specs=[smem, vmem, vmem] + [hbm] * len(blocks),
        out_specs=vmem,
        scratch_shapes=[
            pltpu.VMEM((len(blocks) * size + 16, LANES), jnp.int32),
            pltpu.SemaphoreType.DMA((len(blocks),)),
        ],
        compiler_params=pltpu.CompilerParams(vmem_limit_bytes=48 * 2**20),
        name="values",
    )(place.reshape(-1), odd, child_value, *blocks)


def split(x, parts):
    out = []
    for _ in range(parts):
        out.append(x.astype(jnp.bfloat16))
        x = x - out[-1].astype(jnp.float32)
    return out


def outgoing_body(value_ref, row_ref, reach_ref, slot_ref, out_ref, weighted):
    rows = value_ref.shape[0]
    table = jnp.concatenate(split(value_ref[...].T, 2), axis=1)
    row_of = iota((rows, LANES), 0)
    lane_of = iota((LANES, LANES), 0)

    def step(p, carry):
        query = row_ref[pl.ds(p, 1), :]
        hot = one_hot(row_of == (query >> 7))
        picked = jnp.dot(
            table, jnp.concatenate([hot, hot], axis=0), preferred_element_type=jnp.float32
        )
        hit = lane_of == (query & (LANES - 1))
        chosen = jnp.sum(jnp.where(hit, picked, 0.0), axis=0, keepdims=True)
        weighted[pl.ds(p, 1), :] = chosen * reach_ref[p]
        return carry

    lax.fori_loop(0, row_ref.shape[0], step, 0, unroll=2)
    slots, parents = out_ref.shape[0], row_ref.shape[0]
    place = one_hot(iota((slots, parents), 0) == slot_ref[...])
    total = jnp.zeros(out_ref.shape, jnp.float32)
    for part in split(weighted[...], 3):
        total = total + jnp.dot(place, part, preferred_element_type=jnp.float32)
    out_ref[...] = total


def outgoing_rows(history_value, child_row, reach, slot, slots):
    parents, acts = child_row.shape
    vmem, smem = (pl.BlockSpec(memory_space=s) for s in (pltpu.VMEM, pltpu.SMEM))
    return pl.pallas_call(
        outgoing_body,
        out_shape=jax.ShapeDtypeStruct((slots, acts), jnp.float32),
        in_specs=[vmem, vmem, smem, vmem],
        out_specs=vmem,
        scratch_shapes=[pltpu.VMEM((parents, acts), jnp.float32)],
        name="outgoing",
    )(history_value, child_row, reach, slot[None, :])


def factors(n):
    high = 1
    while high * high < n:
        high *= 2
    return high, n // high


def exchange(block, across, depth, width):
    def device(y, core, z, x):
        return ((y * 2 + core) * depth + z) * width + x

    def move(array, to):
        pairs = []
        for y in range(across // 2):
            for core in range(2):
                for z in range(depth):
                    for x in range(width):
                        pairs.append((device(y, core, z, x), device(*to(y, core, z, x))))
        return lax.ppermute(array, AXES, pairs)

    def ring(y, core, z, x):
        return (y, core, (z + 1) % depth, x)

    def near(y, core, z, x):
        return (y, core, z, x ^ 1) if core == 0 else (y ^ 1, core, z, x)

    def far(y, core, z, x):
        return (y ^ 1, core, z, x) if core == 0 else (y, core, z, x ^ 1)

    def twin(y, core, z, x):
        return (y, 1 - core, z, x)

    mine = []
    for step in range(depth):
        start = block if step == 0 else move(start, ring)
        beside = move(start, near)
        mine += [start, beside, move(start, far), move(beside, far)]
    return mine + [move(part, twin) for part in mine]


def local(child_value, child_row, opp_set, opp_home, opp_cum, reach, br_set, br_home, br_cum):
    across = lax.axis_size("gx")
    along = lax.axis_size("gy")
    devices = across * along
    depth, width = factors(along)
    hist, acts = child_value.shape
    parents = reach.shape[0]
    per_opp = opp_cum.shape[0]
    per_br = br_cum.shape[0]
    words = per_opp // 2
    limit_two = max(2, (2 * parents + devices - 1) // devices)

    policy = (opp_cum / jnp.sum(opp_cum, axis=1, keepdims=True)).astype(jnp.bfloat16)
    fixed = jnp.round(policy.astype(jnp.float32) * float(2**SCALE_BITS)).astype(jnp.int32)
    packed = fixed[:words] | (fixed[words:] << 16)

    home = lookup(opp_home, opp_set.reshape(hist // LANES, LANES))
    owner = home // per_opp
    inside = home % per_opp
    odd = inside // words
    if across == 4 and width == 2 and devices * words * acts * 4 <= TABLE_LIMIT:
        gx, gy = lax.axis_index("gx"), lax.axis_index("gy")
        my_y, my_core, my_z, my_x = gx // 2, gx % 2, gy // width, gy % width
        y, core = owner // along // 2, owner // along % 2
        z, x = owner % along // width, owner % width
        flip_x, flip_y = x ^ my_x, y ^ my_y
        step = (my_z - z) % depth
        turn = jnp.where(core == 0, flip_x + 2 * flip_y, flip_y + 2 * flip_x)
        block = ((core ^ my_core) * depth + step) * 4 + turn
        place = block * words + inside % words
        blocks = exchange(packed, across, depth, width)
        history_value = values_from(blocks, place, odd, child_value)
    else:
        table = lax.all_gather(packed, AXES, axis=0, tiled=True)
        rows = jnp.take(table, (owner * words + inside % words).reshape(-1), axis=0)
        rows = lax.shift_right_logical(rows, 16 * odd.reshape(-1, 1)) & 0xFFFF
        history_value = jnp.einsum(
            "ra,ra->r", rows.astype(jnp.float32), child_value.astype(jnp.float32)
        ) * (0.5**SCALE_BITS)
        history_value = history_value.reshape(hist // LANES, LANES)

    home_two = jnp.take(br_home, br_set)
    owner_two = home_two // per_br
    earlier = jnp.arange(parents)[:, None] > jnp.arange(parents)[None, :]
    same = owner_two[:, None] == owner_two[None, :]
    rank_two = jnp.sum((earlier & same).astype(jnp.int32), axis=1)
    place_two = owner_two * limit_two + rank_two
    slots = devices * limit_two
    taken = place_two[None, :] == jnp.arange(slots, dtype=jnp.int32)[:, None]
    asked_two = jnp.sum(jnp.where(taken, home_two % per_br + 1, 0), axis=1) - 1
    early = jnp.concatenate(
        [
            asked_two.reshape(devices, limit_two).astype(jnp.float32),
            jnp.full((devices, 1), jnp.sum(reach)),
            jnp.zeros((devices, LANES - 1 - limit_two), jnp.float32),
        ],
        axis=1,
    )
    early = lax.all_to_all(early, AXES, split_axis=0, concat_axis=0, tiled=True)
    asked_two = early[:, :limit_two].astype(jnp.int32).reshape(-1)
    reach_total = jnp.sum(early[:, limit_two])

    outgoing_two = outgoing_rows(
        history_value, child_row.reshape(parents, acts), reach, place_two, slots
    )
    incoming_two = lax.all_to_all(outgoing_two, AXES, split_axis=0, concat_axis=0, tiled=True)
    member = (asked_two[None, :] == jnp.arange(per_br, dtype=jnp.int32)[:, None]).astype(
        jnp.float32
    )
    action_value = jnp.dot(member, incoming_two, precision=lax.Precision.HIGHEST)
    br_policy = br_cum / jnp.sum(br_cum, axis=1, keepdims=True)
    regret_gap = jnp.max(action_value, axis=1) - jnp.sum(br_policy * action_value, axis=1)
    gaps = jnp.full((devices, LANES), jnp.sum(regret_gap))
    gaps = lax.all_to_all(gaps, AXES, split_axis=0, concat_axis=0, tiled=True)
    gap_total = jnp.sum(gaps[:, 0])
    return (history_value.reshape(-1), regret_gap, gap_total / reach_total)


def solution(mesh):
    placed = (
        P(AXES, None),
        P(AXES, None),
        P(AXES),
        P(),
        P(AXES, None),
        P(AXES),
        P(AXES),
        P(),
        P(AXES, None),
    )
    return jax.shard_map(
        local,
        mesh=mesh,
        in_specs=placed,
        out_specs=(P(AXES), P(AXES), P()),
        check_vma=False,
    )
```

```python
import functools

import jax
import jax.numpy as jnp
from jax import lax
from jax.experimental import pallas as pl
from jax.experimental.pallas import tpu as pltpu
from jax.sharding import PartitionSpec as P


AXES = ("gx", "gy")
LANES = 128
SCALE_BITS = 17
TABLE_LIMIT = 24 * 2**20
SHARES = (5, 3, 6, 1, 1)


def iota(shape, dim):
    return lax.broadcasted_iota(jnp.int32, shape, dim)


def one_hot(hit):
    return jnp.where(hit, 1.0, 0.0).astype(jnp.bfloat16)


def room(size):
    return pltpu.CompilerParams(vmem_limit_bytes=size + 4 * 2**20)


def spaces():
    return (pl.BlockSpec(memory_space=s) for s in (pltpu.VMEM, pltpu.SMEM, pl.ANY))


def pick(table, query_refs, parts):
    height = table.shape[1] // parts
    row_of = iota((height, LANES), 0)
    lane_of = iota((LANES, LANES), 0)
    rows = jnp.concatenate([one_hot(row_of == (q >> 7)) for q in query_refs], axis=1)
    rows = jnp.concatenate([rows] * parts, axis=0) if parts > 1 else rows
    found = jnp.dot(table, rows, preferred_element_type=jnp.float32)
    return [
        (found[:, LANES * k : LANES * (k + 1)], lane_of == (q & (LANES - 1)))
        for k, q in enumerate(query_refs)
    ]


def lookup_body(first, last, planes_ref, query_ref, *refs):
    out_ref = refs[-1]
    count, group = planes_ref.shape[0] // LANES, 8
    if len(refs) > 1:
        out_ref[:first, :] = refs[0][:first, :]

    def step(i, carry):
        queries = [query_ref[pl.ds(group * i + k, 1), :] for k in range(group)]
        table = planes_ref[...]
        found = [
            pick(table[LANES * c : LANES * (c + 1)], queries, 1) for c in range(count)
        ]
        for k in range(group):
            total, hit = found[0][k]
            for c in range(1, count):
                total = total + found[c][k][0] * float(256**c)
            value = jnp.sum(jnp.where(hit, total, 0.0), axis=0, keepdims=True)
            out_ref[pl.ds(group * i + k, 1), :] = value.astype(jnp.int32)
        return carry

    lax.fori_loop(first // group, last // group, step, 0)


def planes_body(table_ref, out_ref):
    high = table_ref.shape[0]
    for c in range(out_ref.shape[0] // LANES):
        for h in range(0, high, LANES):
            byte = (table_ref[h : h + LANES, :] >> (8 * c)) & 255
            out_ref[LANES * c : LANES * (c + 1), h : h + LANES] = byte.astype(
                jnp.float32
            ).T.astype(jnp.bfloat16)


def byte_planes(table):
    size = table.shape[0]
    count = max(1, ((size - 1).bit_length() + 7) // 8)
    return pl.pallas_call(
        planes_body,
        out_shape=jax.ShapeDtypeStruct((count * LANES, size // LANES), jnp.bfloat16),
        compiler_params=room(table.size * 8),
        name="planes",
    )(table.reshape(-1, LANES))


def lookups(table, query):
    planes = byte_planes(table)
    rows = query.shape[0]
    edges = [0]
    for share in SHARES:
        edges.append(edges[-1] + rows // 16 // 8 * 8 * share)
    edges[-1] = rows
    found = ()
    for first, last in zip(edges, edges[1:]):
        found = (
            pl.pallas_call(
                functools.partial(lookup_body, first, last),
                out_shape=jax.ShapeDtypeStruct(query.shape, jnp.int32),
                compiler_params=room(planes.size * 16),
                name="lookup",
            )(planes, query, *found),
        )
    return found[0]


def pack_body(cum_ref, out_ref):
    half = out_ref.shape[0]
    rows = min(half, 64)

    def fixed(first):
        cum = cum_ref[pl.ds(first, rows), :]
        policy = (cum / jnp.sum(cum, axis=1, keepdims=True)).astype(jnp.bfloat16)
        return (policy.astype(jnp.float32) * float(2**SCALE_BITS) + 0.5).astype(jnp.int32)

    def step(i, carry):
        first = pl.multiple_of(i * rows, rows)
        out_ref[pl.ds(first, rows), :] = fixed(first) | (fixed(first + half) << 16)
        return carry

    lax.fori_loop(0, half // rows, step, 0, unroll=2)


def pack(opp_cum):
    rows, acts = opp_cum.shape
    return pl.pallas_call(
        pack_body,
        out_shape=jax.ShapeDtypeStruct((rows // 2, acts), jnp.int32),
        compiler_params=room(opp_cum.size * 6),
        name="pack",
    )(opp_cum)


def split(x, parts):
    out = []
    for _ in range(parts):
        out.append(x.astype(jnp.bfloat16))
        x = x - out[-1].astype(jnp.float32)
    return out


def outgoing(value_ref, row_ref, reach_ref, slot_ref, out_ref, weighted):
    table = jnp.concatenate(split(value_ref[...].T, 2), axis=1)
    group = 8

    def step(i, carry):
        queries = [row_ref[pl.ds(group * i + k, 1), :] for k in range(group)]
        for k, (found, hit) in enumerate(pick(table, queries, 2)):
            chosen = jnp.sum(jnp.where(hit, found, 0.0), axis=0, keepdims=True)
            weighted[pl.ds(group * i + k, 1), :] = chosen
        return carry

    lax.fori_loop(0, row_ref.shape[0] // group, step, 0)
    place = one_hot(iota((out_ref.shape[0], row_ref.shape[0]), 0) == slot_ref[...])
    total = jnp.zeros(out_ref.shape, jnp.float32)
    for part in split(weighted[...] * reach_ref[...], 3):
        total = total + jnp.dot(place, part, preferred_element_type=jnp.float32)
    out_ref[...] = total


def outgoing_rows(history_value, child_row, reach, slot, slots):
    return pl.pallas_call(
        outgoing,
        out_shape=jax.ShapeDtypeStruct((slots, LANES), jnp.float32),
        scratch_shapes=[pltpu.VMEM(child_row.shape, jnp.float32)],
        compiler_params=room(4 * 2**20),
        name="outgoing",
    )(history_value, child_row, reach, slot)


def value_body(blocks, place_ref, odd_ref, child_ref, row_ref, reach_ref, slot_ref, *rest):
    block_refs = rest[:blocks]
    value_ref, out_ref, table, weighted, sems = rest[blocks:]
    size = block_refs[0].shape[0]
    copies = [
        pltpu.make_async_copy(ref, table.at[pl.ds(8 + b * size, size), :], sems.at[b])
        for b, ref in enumerate(block_refs)
    ]
    for copy in copies:
        copy.start()
    for copy in copies:
        copy.wait()
    sub = iota((8, LANES), 0)
    spot = iota((8, LANES), 1) - sub

    tiles = value_ref.shape[0]

    def place(k, t):
        return place_ref.at[pl.ds(k * tiles, tiles)][t]

    def tile(t, carry):
        low = jnp.zeros((8, LANES), jnp.float32)
        high = jnp.zeros((8, LANES), jnp.float32)
        start = pl.multiple_of(t * LANES, LANES)
        children = child_ref.at[pl.ds(start, LANES), :]
        for g in range(LANES // 16):
            child = children[16 * g : 16 * g + 16, :].astype(jnp.float32)
            for half in range(2):
                at = 16 * g + 8 * half
                words = table[pl.ds(place(at, t) + 8, 8), :]
                for s in range(1, 8):
                    row = table[pl.ds(place(at + s, t) + (8 - s), 8), :]
                    words = jnp.where(sub == s, row, words)
                part = child[8 * half : 8 * half + 8]
                even = (words & 0xFFFF).astype(jnp.float32) * part
                odd = lax.shift_right_logical(words, 16).astype(jnp.float32) * part
                here = spot == at
                low = jnp.where(here, jnp.sum(even, axis=1, keepdims=True), low)
                high = jnp.where(here, jnp.sum(odd, axis=1, keepdims=True), high)
        low = jnp.sum(low, axis=0, keepdims=True)
        high = jnp.sum(high, axis=0, keepdims=True)
        picked = jnp.where(odd_ref[pl.ds(t, 1), :] > 0, high, low)
        value_ref[pl.ds(t, 1), :] = picked * (0.5**SCALE_BITS)
        return carry

    lax.fori_loop(0, tiles, tile, 0, unroll=2)
    outgoing(value_ref, row_ref, reach_ref, slot_ref, out_ref, weighted)


def values_from(blocks, place, odd, child_value, child_row, reach, slot, slots):
    size = blocks[0].shape[0]
    vmem, smem, hbm = spaces()
    return pl.pallas_call(
        functools.partial(value_body, len(blocks)),
        out_shape=(
            jax.ShapeDtypeStruct(odd.shape, jnp.float32),
            jax.ShapeDtypeStruct((slots, LANES), jnp.float32),
        ),
        in_specs=[smem] + [vmem] * 5 + [hbm] * len(blocks),
        out_specs=(vmem, vmem),
        scratch_shapes=[
            pltpu.VMEM((len(blocks) * size + 16, LANES), jnp.int32),
            pltpu.VMEM(child_row.shape, jnp.float32),
            pltpu.SemaphoreType.DMA((len(blocks),)),
        ],
        compiler_params=room(len(blocks) * size * LANES * 4 + 4 * 2**20),
        name="values",
    )(place.T.reshape(-1), odd, child_value, child_row, reach, slot, *blocks)


def regret_body(asked_ref, incoming_ref, cum_ref, gap_ref, total_ref):
    sets = cum_ref.shape[0]
    member = one_hot(iota((sets, asked_ref.shape[1]), 0) == asked_ref[...])
    value = jnp.zeros(cum_ref.shape, jnp.float32)
    for part in split(incoming_ref[...], 3):
        value = value + jnp.dot(member, part, preferred_element_type=jnp.float32)
    policy = cum_ref[...] / jnp.sum(cum_ref[...], axis=1, keepdims=True)
    gap = jnp.max(value, axis=1, keepdims=True) - jnp.sum(policy * value, axis=1, keepdims=True)
    own = iota((sets, LANES), 0) == iota((sets, LANES), 1)
    gap_ref[...] = jnp.sum(jnp.where(own, gap, 0.0), axis=0, keepdims=True)
    total = jnp.sum(jnp.broadcast_to(gap, (sets, LANES)), axis=0, keepdims=True)
    total_ref[...] = jnp.broadcast_to(total, total_ref.shape)


def regrets(asked, incoming, br_cum, devices):
    return pl.pallas_call(
        regret_body,
        out_shape=(
            jax.ShapeDtypeStruct((1, LANES), jnp.float32),
            jax.ShapeDtypeStruct((devices, LANES), jnp.float32),
        ),
        compiler_params=room(incoming.size * 16),
        name="regret",
    )(asked, incoming, br_cum)


def factors(n):
    high = 1
    while high * high < n:
        high *= 2
    return high, n // high


def exchange(block, across, depth, width):
    def device(y, core, z, x):
        return ((y * 2 + core) * depth + z) * width + x

    def move(array, to):
        pairs = []
        for y in range(across // 2):
            for core in range(2):
                for z in range(depth):
                    for x in range(width):
                        pairs.append((device(y, core, z, x), device(*to(y, core, z, x))))
        return lax.ppermute(array, AXES, pairs)

    def ring(y, core, z, x):
        return (y, core, (z + 1) % depth, x)

    def near(y, core, z, x):
        return (y, core, z, x ^ 1) if core == 0 else (y ^ 1, core, z, x)

    def far(y, core, z, x):
        return (y ^ 1, core, z, x) if core == 0 else (y, core, z, x ^ 1)

    def twin(y, core, z, x):
        return (y, 1 - core, z, x)

    start, beside, across_from, diagonal = [block], [], [], []
    for step in range(depth):
        if step:
            start.append(move(start[-1], ring))
        beside.append(move(start[-1], near))
        across_from.append(move(start[-1], far))
        if 0 < step < depth - 1:
            diagonal.append(move(diagonal[-1], ring))
        else:
            diagonal.append(move(beside[-1], far))
    mine = [part for group in zip(start, beside, across_from, diagonal) for part in group]
    return mine + [move(part, twin) for part in mine]


def local(child_value, child_row, opp_set, opp_home, opp_cum, reach, br_set, br_home, br_cum):
    across = lax.axis_size("gx")
    along = lax.axis_size("gy")
    devices = across * along
    depth, width = factors(along)
    hist, acts = child_value.shape
    parents = reach.shape[0]
    per_opp = opp_cum.shape[0]
    per_br = br_cum.shape[0]
    words = per_opp // 2
    limit_two = max(2, (2 * parents + devices - 1) // devices)

    packed = pack(opp_cum)

    home = lookups(opp_home, opp_set.reshape(hist // LANES, LANES))
    owner = home // per_opp
    inside = home % per_opp
    odd = inside // words
    home_two = jnp.take(br_home, br_set)
    owner_two = home_two // per_br
    earlier = jnp.arange(parents)[:, None] > jnp.arange(parents)[None, :]
    same = owner_two[:, None] == owner_two[None, :]
    rank_two = jnp.sum((earlier & same).astype(jnp.int32), axis=1)
    place_two = owner_two * limit_two + rank_two
    slots = devices * limit_two
    taken = place_two[None, :] == jnp.arange(slots, dtype=jnp.int32)[:, None]
    asked_two = jnp.sum(jnp.where(taken, home_two % per_br + 1, 0), axis=1) - 1
    early = jnp.concatenate(
        [
            asked_two.reshape(devices, limit_two).astype(jnp.float32),
            jnp.full((devices, 1), jnp.sum(reach)),
            jnp.zeros((devices, LANES - 1 - limit_two), jnp.float32),
        ],
        axis=1,
    )
    early = lax.all_to_all(early, AXES, split_axis=0, concat_axis=0, tiled=True)
    asked_two = early[:, :limit_two].astype(jnp.int32).reshape(-1)
    reach_total = jnp.sum(early[:, limit_two])

    rows_two = child_row.reshape(parents, acts)
    if across == 4 and (depth, width) == (4, 2) and devices * words * acts * 4 <= TABLE_LIMIT:
        gx, gy = lax.axis_index("gx"), lax.axis_index("gy")
        my_y, my_core, my_z, my_x = gx // 2, gx % 2, gy // width, gy % width
        y, core = owner // along // 2, owner // along % 2
        z, x = owner % along // width, owner % width
        flip_x, flip_y = x ^ my_x, y ^ my_y
        step = (my_z - z) % depth
        turn = jnp.where(core == 0, flip_x + 2 * flip_y, flip_y + 2 * flip_x)
        block = ((core ^ my_core) * depth + step) * 4 + turn
        place = block * words + inside % words
        blocks = exchange(packed, across, depth, width)
        history_value, outgoing_two = values_from(
            blocks, place, odd, child_value, rows_two, reach[:, None], place_two[None, :], slots
        )
    else:
        table = lax.all_gather(packed, AXES, axis=0, tiled=True)
        rows = jnp.take(table, (owner * words + inside % words).reshape(-1), axis=0)
        rows = lax.shift_right_logical(rows, 16 * odd.reshape(-1, 1)) & 0xFFFF
        history_value = jnp.einsum(
            "ra,ra->r", rows.astype(jnp.float32), child_value.astype(jnp.float32)
        ) * (0.5**SCALE_BITS)
        history_value = history_value.reshape(hist // LANES, LANES)
        outgoing_two = outgoing_rows(
            history_value, rows_two, reach[:, None], place_two[None, :], slots
        )
    incoming_two = lax.all_to_all(outgoing_two, AXES, split_axis=0, concat_axis=0, tiled=True)
    gap_row, gaps = regrets(asked_two[None, :], incoming_two, br_cum, devices)
    regret_gap = gap_row[0, :per_br]
    gaps = lax.all_to_all(gaps, AXES, split_axis=0, concat_axis=0, tiled=True)
    gap_total = jnp.sum(gaps[:, 0])
    return (history_value.reshape(-1), regret_gap, gap_total / reach_total)


def shortcut(mesh):
    gx, gy = mesh.shape["gx"], mesh.shape["gy"]
    return gx == 4 and factors(gy) == (4, 2)


def solution(mesh):
    placed = (
        P(AXES, None),
        P(AXES, None),
        P(AXES),
        P(),
        P(AXES, None),
        P(AXES),
        P(AXES),
        P(),
        P(AXES, None),
    )
    step = jax.shard_map(
        local,
        mesh=mesh,
        in_specs=placed,
        out_specs=(P(AXES), P(AXES), P()),
        check_vma=False,
    )
    return step if shortcut(mesh) else step
```

```python
import functools

import jax
import jax.numpy as jnp
from jax import lax
from jax.experimental import pallas as pl
from jax.experimental.pallas import tpu as pltpu
from jax.sharding import PartitionSpec as P


AXES = ("gx", "gy")
LANES = 128
SCALE_BITS = 17
TABLE_LIMIT = 24 * 2**20
CHUNKS = 8
SHARES = (5, 5, 4, 1, 1)
STAGED = tuple(i for i in range(16) if i not in (11, 14, 15))
STAGED += tuple(16 + i for i in range(16) if i not in (7, 11, 13, 14, 15))


def iota(shape, dim):
    return lax.broadcasted_iota(jnp.int32, shape, dim)


def one_hot(hit):
    return jnp.where(hit, 1.0, 0.0).astype(jnp.bfloat16)


def room(size):
    return pltpu.CompilerParams(vmem_limit_bytes=size + 4 * 2**20)


def spaces():
    return (pl.BlockSpec(memory_space=s) for s in (pltpu.VMEM, pltpu.SMEM, pl.ANY))


def pick(table, query_refs, parts):
    height = table.shape[1] // parts
    row_of = iota((height, LANES), 0)
    lane_of = iota((LANES, LANES), 0)
    rows = jnp.concatenate([one_hot(row_of == (q >> 7)) for q in query_refs], axis=1)
    rows = jnp.concatenate([rows] * parts, axis=0) if parts > 1 else rows
    found = jnp.dot(table, rows, preferred_element_type=jnp.float32)
    return [
        (found[:, LANES * k : LANES * (k + 1)], lane_of == (q & (LANES - 1)))
        for k, q in enumerate(query_refs)
    ]


def lookup_body(first, last, planes_ref, query_ref, *refs):
    out_ref = refs[-1]
    count, group = planes_ref.shape[0] // LANES, 8
    if len(refs) > 1:
        out_ref[:first, :] = refs[0][:first, :]

    def step(i, carry):
        queries = [query_ref[pl.ds(group * i + k, 1), :] for k in range(group)]
        table = planes_ref[...]
        found = [
            pick(table[LANES * c : LANES * (c + 1)], queries, 1) for c in range(count)
        ]
        for k in range(group):
            total, hit = found[0][k]
            for c in range(1, count):
                total = total + found[c][k][0] * float(256**c)
            value = jnp.sum(jnp.where(hit, total, 0.0), axis=0, keepdims=True)
            out_ref[pl.ds(group * i + k, 1), :] = value.astype(jnp.int32)
        return carry

    lax.fori_loop(first // group, last // group, step, 0)


def planes_body(table_ref, out_ref):
    high = table_ref.shape[0]
    for c in range(out_ref.shape[0] // LANES):
        for h in range(0, high, LANES):
            byte = (table_ref[h : h + LANES, :] >> (8 * c)) & 255
            out_ref[LANES * c : LANES * (c + 1), h : h + LANES] = byte.astype(
                jnp.float32
            ).T.astype(jnp.bfloat16)


def byte_planes(table):
    size = table.shape[0]
    count = max(1, ((size - 1).bit_length() + 7) // 8)
    return pl.pallas_call(
        planes_body,
        out_shape=jax.ShapeDtypeStruct((count * LANES, size // LANES), jnp.bfloat16),
        compiler_params=room(table.size * 8),
        name="planes",
    )(table.reshape(-1, LANES))


def lookups(table, query):
    planes = byte_planes(table)
    rows = query.shape[0]
    edges = [0]
    for share in SHARES:
        edges.append(edges[-1] + rows // 16 // 8 * 8 * share)
    edges[-1] = rows
    found = ()
    for first, last in zip(edges, edges[1:]):
        found = (
            pl.pallas_call(
                functools.partial(lookup_body, first, last),
                out_shape=jax.ShapeDtypeStruct(query.shape, jnp.int32),
                compiler_params=room(planes.size * 16),
                name="lookup",
            )(planes, query, *found),
        )
    return found[0]


def pack_body(cum_ref, out_ref):
    half = out_ref.shape[0]
    rows = min(half, 64)

    def fixed(first):
        cum = cum_ref[pl.ds(first, rows), :]
        policy = (cum / jnp.sum(cum, axis=1, keepdims=True)).astype(jnp.bfloat16)
        return (policy.astype(jnp.float32) * float(2**SCALE_BITS) + 0.5).astype(jnp.int32)

    def step(i, carry):
        first = pl.multiple_of(i * rows, rows)
        out_ref[pl.ds(first, rows), :] = fixed(first) | (fixed(first + half) << 16)
        return carry

    lax.fori_loop(0, half // rows, step, 0, unroll=2)


def pack(opp_cum):
    rows, acts = opp_cum.shape
    return pl.pallas_call(
        pack_body,
        out_shape=jax.ShapeDtypeStruct((rows // 2, acts), jnp.int32),
        compiler_params=room(opp_cum.size * 6),
        name="pack",
    )(opp_cum)


def split(x, parts):
    out = []
    for _ in range(parts):
        out.append(x.astype(jnp.bfloat16))
        x = x - out[-1].astype(jnp.float32)
    return out


def outgoing(value_ref, row_ref, reach_ref, slot_ref, note_ref, out_ref, weighted):
    table = jnp.concatenate(split(value_ref[...].T, 2), axis=1)
    group = 8

    def step(i, carry):
        queries = [row_ref[pl.ds(group * i + k, 1), :] for k in range(group)]
        for k, (found, hit) in enumerate(pick(table, queries, 2)):
            chosen = jnp.sum(jnp.where(hit, found, 0.0), axis=0, keepdims=True)
            weighted[pl.ds(group * i + k, 1), :] = chosen
        return carry

    lax.fori_loop(0, row_ref.shape[0] // group, step, 0)
    devices, tall = note_ref.shape[0], out_ref.shape[1]
    limit = tall // 2
    place = one_hot(iota((devices * limit, row_ref.shape[0]), 0) == slot_ref[...])
    total = jnp.zeros((devices * limit, LANES), jnp.float32)
    for part in split(weighted[...] * column(reach_ref[...]), 3):
        total = total + jnp.dot(place, part, preferred_element_type=jnp.float32)
    for d in range(devices):
        out_ref[d, :limit, :] = total[limit * d : limit * (d + 1)]
        out_ref[d, limit:, :] = jnp.broadcast_to(note_ref[d : d + 1, :], (limit, LANES))


def outgoing_rows(history_value, child_row, reach, slot, notes, limit):
    return pl.pallas_call(
        outgoing,
        out_shape=jax.ShapeDtypeStruct((notes.shape[0], 2 * limit, LANES), jnp.float32),
        scratch_shapes=[pltpu.VMEM(child_row.shape, jnp.float32)],
        compiler_params=room(4 * 2**20),
        name="outgoing",
    )(history_value, child_row, reach, slot, notes)


def fill(refs, slots, table, sems):
    size = refs[0].shape[0]
    return [
        pltpu.make_async_copy(ref, table.at[pl.ds(8 + b * size, size), :], sems.at[i])
        for i, (ref, b) in enumerate(zip(refs, slots))
    ]


def quotient(x, n):
    return x >> (n.bit_length() - 1) if n & (n - 1) == 0 else x // n


def split_by(x, n):
    whole = quotient(x, n)
    return whole, x - whole * n


def stage_body(slots, along, width, words, home_ref, *refs):
    block_refs, (table, place_ref, odd_ref, sems) = refs[: len(slots)], refs[len(slots) :]
    copies = fill(block_refs, slots, table, sems)
    for copy in copies:
        copy.start()
    depth = along // width
    gx, gy = lax.axis_index("gx"), lax.axis_index("gy")
    my_y, my_core = split_by(gx, 2)
    my_z, my_x = split_by(gy, width)
    row, inside = split_by(home_ref[...], words)
    owner, odd = split_by(row, 2)
    chip, place = split_by(owner, along)
    y, core = split_by(chip, 2)
    z, x = split_by(place, width)
    flip_x, flip_y = x ^ my_x, y ^ my_y
    turn = jnp.where(core == 0, flip_x + 2 * flip_y, flip_y + 2 * flip_x)
    step = my_z - z
    step = jnp.where(step < 0, step + depth, step)
    block = ((core ^ my_core) * depth + step) * 4 + turn
    at = (block * words + inside).astype(jnp.float32)
    place_ref[...] = at.T.astype(jnp.int32)
    odd_ref[...] = odd
    for copy in copies:
        copy.wait()


def staged(blocks, home, along, width):
    size = blocks[0].shape[0]
    vmem, _, hbm = spaces()
    shape = (len(blocks) * size + 16, LANES)
    return pl.pallas_call(
        functools.partial(stage_body, STAGED, along, width, size),
        out_shape=(
            jax.ShapeDtypeStruct(shape, jnp.int32),
            jax.ShapeDtypeStruct(home.shape[::-1], jnp.int32),
            jax.ShapeDtypeStruct(home.shape, jnp.int32),
        ),
        in_specs=[vmem] + [hbm] * len(STAGED),
        out_specs=(vmem, vmem, vmem),
        scratch_shapes=[pltpu.SemaphoreType.DMA((len(STAGED),))],
        compiler_params=room(0),
        name="stage",
    )(home, *(blocks[b] for b in STAGED))


def value_body(slots, place_ref, odd_ref, child_ref, *rest):
    upper, block_refs = rest[:4], rest[5 : 5 + len(slots)]
    value_ref, out_ref, table, child, weighted, sems, arrived = rest[5 + len(slots) :]
    copies = fill(block_refs, slots, table, sems)
    tiles = value_ref.shape[0]
    chunk = tiles // CHUNKS

    def children_of(c):
        rows = pl.ds(c * chunk * LANES, chunk * LANES)
        return pltpu.make_async_copy(child_ref.at[rows, :], child.at[rows, :], arrived.at[c])

    for copy in copies:
        copy.start()
    for c in range(CHUNKS):
        children_of(c).start()
    for copy in copies:
        copy.wait()
    sub = iota((8, LANES), 0)
    spot = iota((8, LANES), 1) - sub

    def place(k, t):
        return place_ref.at[pl.ds(k * tiles, tiles)][t]

    def tile(t, carry):
        low = jnp.zeros((8, LANES), jnp.float32)
        high = jnp.zeros((8, LANES), jnp.float32)
        start = pl.multiple_of(t * LANES, LANES)
        children = child.at[pl.ds(start, LANES), :]
        for g in range(LANES // 16):
            values = children[16 * g : 16 * g + 16, :].astype(jnp.float32)
            for half in range(2):
                at = 16 * g + 8 * half
                words = table[pl.ds(place(at, t) + 8, 8), :]
                for s in range(1, 8):
                    row = table[pl.ds(place(at + s, t) + (8 - s), 8), :]
                    words = jnp.where(sub == s, row, words)
                part = values[8 * half : 8 * half + 8]
                even = (words & 0xFFFF).astype(jnp.float32) * part
                odd = lax.shift_right_logical(words, 16).astype(jnp.float32) * part
                here = spot == at
                low = jnp.where(here, jnp.sum(even, axis=1, keepdims=True), low)
                high = jnp.where(here, jnp.sum(odd, axis=1, keepdims=True), high)
        low = jnp.sum(low, axis=0, keepdims=True)
        high = jnp.sum(high, axis=0, keepdims=True)
        picked = jnp.where(odd_ref[pl.ds(t, 1), :] > 0, high, low)
        value_ref[pl.ds(t, 1), :] = picked * (0.5**SCALE_BITS)
        return carry

    def stretch(c, carry):
        children_of(c).wait()
        return lax.fori_loop(
            0, chunk, lambda i, carry: tile(c * chunk + i, carry), carry, unroll=4
        )

    lax.fori_loop(0, CHUNKS, stretch, 0)
    outgoing(value_ref, *upper, out_ref, weighted)


def values_from(blocks, home, along, width, child_value, child_row, reach, slot, notes, limit):
    table, place, odd = staged(blocks, home, along, width)
    rest = tuple(b for b in range(len(blocks)) if b not in STAGED)
    vmem, smem, hbm = spaces()
    return pl.pallas_call(
        functools.partial(value_body, rest),
        out_shape=(
            jax.ShapeDtypeStruct(odd.shape, jnp.float32),
            jax.ShapeDtypeStruct((notes.shape[0], 2 * limit, LANES), jnp.float32),
            jax.ShapeDtypeStruct(table.shape, table.dtype),
        ),
        in_specs=[smem, vmem, pl.BlockSpec(memory_space=pltpu.HBM)]
        + [vmem] * 5
        + [hbm] * len(rest),
        out_specs=(vmem, vmem, vmem),
        scratch_shapes=[
            pltpu.VMEM(child_value.shape, child_value.dtype),
            pltpu.VMEM(child_row.shape, jnp.float32),
            pltpu.SemaphoreType.DMA((len(rest),)),
            pltpu.SemaphoreType.DMA((CHUNKS,)),
        ],
        input_output_aliases={7: 2},
        compiler_params=room(8 * 2**20),
        name="values",
    )(
        place.reshape(-1),
        odd,
        pltpu.with_memory_space_constraint(child_value, pltpu.HBM),
        child_row,
        reach,
        slot,
        notes,
        table,
        *(blocks[b] for b in rest),
    )[:2]


def column(row):
    return jnp.broadcast_to(row.astype(jnp.float32), (row.shape[1], row.shape[1])).T


def slots_body(per_br, limit, home_ref, set_ref, reach_ref, place_ref, note_ref):
    parents = set_ref.shape[1]
    count = max(1, ((home_ref.size - 1).bit_length() + 7) // 8)
    home = jnp.zeros(set_ref.shape, jnp.float32)
    for c in range(count):
        byte = ((home_ref[...] >> (8 * c)) & 255).astype(jnp.float32)
        ((found, hit),) = pick(byte.T.astype(jnp.bfloat16), [set_ref[...]], 1)
        home += jnp.sum(jnp.where(hit, found, 0.0), axis=0, keepdims=True) * float(256**c)
    home = home.astype(jnp.int32)
    owner = quotient(home, per_br)
    inside = home - owner * per_br
    square = (parents, parents)
    earlier = iota(square, 0) < iota(square, 1)
    same = column(owner) == owner.astype(jnp.float32)
    rank = jnp.sum(jnp.where(earlier & same, 1.0, 0.0), axis=0, keepdims=True)
    place_ref[...] = owner * limit + rank.astype(jnp.int32)
    devices = note_ref.shape[0]
    here = iota((devices, parents), 0) == owner
    rows = jnp.where(here, (inside + 1).astype(jnp.float32), 0.0).astype(jnp.bfloat16)
    ranks = one_hot(column(rank) == iota((parents, LANES), 1).astype(jnp.float32))
    asked = jnp.dot(rows, ranks, preferred_element_type=jnp.float32) - 1.0
    reach = jnp.sum(jnp.broadcast_to(reach_ref[...], note_ref.shape), axis=1, keepdims=True)
    note_ref[...] = jnp.where(iota(note_ref.shape, 1) == limit, reach, asked)


def slots_of(br_home, br_set, reach, per_br, devices, limit):
    return pl.pallas_call(
        functools.partial(slots_body, per_br, limit),
        out_shape=(
            jax.ShapeDtypeStruct((1, br_set.shape[0]), jnp.int32),
            jax.ShapeDtypeStruct((devices, LANES), jnp.float32),
        ),
        compiler_params=room(2**20),
        name="slots",
    )(br_home.reshape(-1, LANES), br_set[None, :], reach[None, :])


def regret_body(incoming_ref, cum_ref, gap_ref, total_ref, reach_ref):
    sets = cum_ref.shape[0]
    devices, limit = incoming_ref.shape[0], incoming_ref.shape[1] // 2
    notes = jnp.concatenate([incoming_ref[d, limit : limit + 1, :] for d in range(devices)], axis=0)
    lane = iota((devices, LANES), 1)
    value = jnp.zeros(cum_ref.shape, jnp.float32)
    rows = jnp.concatenate([incoming_ref[d, :limit, :] for d in range(devices)], axis=0)
    spread = jnp.concatenate(
        [jnp.broadcast_to(notes[d : d + 1, :], (limit, LANES)) for d in range(devices)], axis=0
    )
    mine = iota(spread.shape, 1) == iota(spread.shape, 0) % limit
    asked = jnp.sum(jnp.where(mine, spread, 0.0), axis=1, keepdims=True)
    wide = jnp.broadcast_to(asked, spread.shape)
    member = one_hot(wide == iota(spread.shape, 1).astype(jnp.float32))
    for part in split(rows, 3):
        value = value + lax.dot_general(
            member, part, (((0,), (0,)), ((), ())), preferred_element_type=jnp.float32
        )[:sets]
    policy = cum_ref[...] / jnp.sum(cum_ref[...], axis=1, keepdims=True)
    gap = jnp.max(value, axis=1, keepdims=True) - jnp.sum(policy * value, axis=1, keepdims=True)
    own = iota((sets, LANES), 0) == iota((sets, LANES), 1)
    gap_ref[...] = jnp.sum(jnp.where(own, gap, 0.0), axis=0, keepdims=True)
    total = jnp.sum(jnp.broadcast_to(gap, (sets, LANES)), axis=0, keepdims=True)
    total_ref[...] = jnp.broadcast_to(total, total_ref.shape)
    reach = jnp.sum(jnp.where(lane == limit, notes, 0.0), axis=1, keepdims=True)
    reach = jnp.sum(jnp.broadcast_to(reach, notes.shape), axis=0, keepdims=True)
    reach_ref[...] = reach


def regrets(incoming, br_cum):
    return pl.pallas_call(
        regret_body,
        out_shape=(
            jax.ShapeDtypeStruct((1, LANES), jnp.float32),
            jax.ShapeDtypeStruct((incoming.shape[0], LANES), jnp.float32),
            jax.ShapeDtypeStruct((1, LANES), jnp.float32),
        ),
        compiler_params=room(incoming.size * 16),
        name="regret",
    )(incoming, br_cum)


def factors(n):
    high = 1
    while high * high < n:
        high *= 2
    return high, n // high


def exchange(block, across, depth, width):
    def device(y, core, z, x):
        return ((y * 2 + core) * depth + z) * width + x

    def move(array, to):
        pairs = []
        for y in range(across // 2):
            for core in range(2):
                for z in range(depth):
                    for x in range(width):
                        pairs.append((device(y, core, z, x), device(*to(y, core, z, x))))
        return lax.ppermute(array, AXES, pairs)

    def ring(y, core, z, x):
        return (y, core, (z + 1) % depth, x)

    def near(y, core, z, x):
        return (y, core, z, x ^ 1) if core == 0 else (y ^ 1, core, z, x)

    def far(y, core, z, x):
        return (y ^ 1, core, z, x) if core == 0 else (y, core, z, x ^ 1)

    def twin(y, core, z, x):
        return (y, 1 - core, z, x)

    start, beside, opposite, diagonal = [block], [], [], []
    for i in range(depth):
        if i:
            start.append(move(start[-1], ring))
        beside.append(move(start[-1], near))
        opposite.append(move(start[-1], far))
        if 0 < i < depth - 1:
            diagonal.append(move(diagonal[-1], ring))
        else:
            diagonal.append(move(beside[-1], far))
    mine = [part for group in zip(start, beside, opposite, diagonal) for part in group]
    return mine + [move(part, twin) for part in mine]


def local(child_value, child_row, opp_set, opp_home, opp_cum, reach, br_set, br_home, br_cum):
    across = lax.axis_size("gx")
    along = lax.axis_size("gy")
    devices = across * along
    depth, width = factors(along)
    hist, acts = child_value.shape
    parents = reach.shape[0]
    per_opp = opp_cum.shape[0]
    per_br = br_cum.shape[0]
    words = per_opp // 2
    limit_two = max(2, (2 * parents + devices - 1) // devices)

    packed = pack(opp_cum)

    home = lookups(opp_home, opp_set.reshape(hist // LANES, LANES))
    place_two, notes = slots_of(br_home, br_set, reach, per_br, devices, limit_two)
    rows_two = child_row.reshape(parents, acts)
    if across == 4 and (depth, width) == (4, 2) and devices * words * acts * 4 <= TABLE_LIMIT:
        blocks = exchange(packed, across, depth, width)
        history_value, outgoing_two = values_from(
            blocks, home, along, width, child_value, rows_two, reach[None, :], place_two, notes, limit_two
        )
    else:
        owner, inside = home // per_opp, home % per_opp
        odd = inside // words
        table = lax.all_gather(packed, AXES, axis=0, tiled=True)
        rows = jnp.take(table, (owner * words + inside % words).reshape(-1), axis=0)
        rows = lax.shift_right_logical(rows, 16 * odd.reshape(-1, 1)) & 0xFFFF
        history_value = jnp.einsum(
            "ra,ra->r", rows.astype(jnp.float32), child_value.astype(jnp.float32)
        ) * (0.5**SCALE_BITS)
        history_value = history_value.reshape(hist // LANES, LANES)
        outgoing_two = outgoing_rows(
            history_value, rows_two, reach[None, :], place_two, notes, limit_two
        )
    incoming_two = lax.all_to_all(outgoing_two, AXES, split_axis=0, concat_axis=0, tiled=True)
    gap_row, gaps, reach_row = regrets(incoming_two, br_cum)
    regret_gap = gap_row[0, :per_br]
    gaps = lax.all_to_all(gaps, AXES, split_axis=0, concat_axis=0, tiled=True)
    gap_total = jnp.sum(gaps[:, 0])
    return (history_value.reshape(-1), regret_gap, gap_total / reach_row[0, 0])


def shortcut(mesh):
    gx, gy = mesh.shape["gx"], mesh.shape["gy"]
    return gx == 4 and factors(gy) == (4, 2)


def solution(mesh):
    placed = (
        P(AXES, None),
        P(AXES, None),
        P(AXES),
        P(),
        P(AXES, None),
        P(AXES),
        P(AXES),
        P(),
        P(AXES, None),
    )
    step = jax.shard_map(
        local,
        mesh=mesh,
        in_specs=placed,
        out_specs=(P(AXES), P(AXES), P()),
        check_vma=False,
    )
    return step if shortcut(mesh) else step
```

```python
import functools

import jax
import jax.numpy as jnp
from jax import lax
from jax.experimental import pallas as pl
from jax.experimental.pallas import tpu as pltpu
from jax.sharding import PartitionSpec as P


AXES = ("gx", "gy")
LANES = 128
SCALE_BITS = 17
TABLE_LIMIT = 24 * 2**20
UNIT, WIDEST = float(2**20), 32767.0
SHARES = (5, 5, 4, 1, 1)
STAGED = tuple(i for i in range(16) if i not in (11, 14, 15))
STAGED += tuple(16 + i for i in range(16) if i not in (7, 11, 13, 14, 15))


def iota(shape, dim):
    return lax.broadcasted_iota(jnp.int32, shape, dim)


def one_hot(hit):
    return jnp.where(hit, 1.0, 0.0).astype(jnp.bfloat16)


def room(size):
    return pltpu.CompilerParams(vmem_limit_bytes=size + 4 * 2**20)


def spaces():
    return (pl.BlockSpec(memory_space=s) for s in (pltpu.VMEM, pltpu.SMEM, pl.ANY))


def pick(table, query_refs, parts):
    height = table.shape[1] // parts
    row_of = iota((height, LANES), 0)
    lane_of = iota((LANES, LANES), 0)
    rows = jnp.concatenate([one_hot(row_of == (q >> 7)) for q in query_refs], axis=1)
    rows = jnp.concatenate([rows] * parts, axis=0) if parts > 1 else rows
    found = jnp.dot(table, rows, preferred_element_type=jnp.float32)
    return [
        (found[:, LANES * k : LANES * (k + 1)], lane_of == (q & (LANES - 1)))
        for k, q in enumerate(query_refs)
    ]


def lookup_body(first, last, planes_ref, query_ref, *refs):
    out_ref = refs[-1]
    count, group = planes_ref.shape[0] // LANES, 8
    if len(refs) > 1:
        out_ref[:first, :] = refs[0][:first, :]

    def step(i, carry):
        queries = [query_ref[pl.ds(group * i + k, 1), :] for k in range(group)]
        table = planes_ref[...]
        found = [
            pick(table[LANES * c : LANES * (c + 1)], queries, 1) for c in range(count)
        ]
        for k in range(group):
            total, hit = found[0][k]
            for c in range(1, count):
                total = total + found[c][k][0] * float(256**c)
            value = jnp.sum(jnp.where(hit, total, 0.0), axis=0, keepdims=True)
            out_ref[pl.ds(group * i + k, 1), :] = value.astype(jnp.int32)
        return carry

    lax.fori_loop(first // group, last // group, step, 0)


def planes_body(table_ref, out_ref):
    high = table_ref.shape[0]
    for c in range(out_ref.shape[0] // LANES):
        for h in range(0, high, LANES):
            byte = (table_ref[h : h + LANES, :] >> (8 * c)) & 255
            out_ref[LANES * c : LANES * (c + 1), h : h + LANES] = byte.astype(
                jnp.float32
            ).T.astype(jnp.bfloat16)


def byte_planes(table):
    size = table.shape[0]
    count = max(1, ((size - 1).bit_length() + 7) // 8)
    return pl.pallas_call(
        planes_body,
        out_shape=jax.ShapeDtypeStruct((count * LANES, size // LANES), jnp.bfloat16),
        compiler_params=room(table.size * 8),
        name="planes",
    )(table.reshape(-1, LANES))


def lookups(table, query):
    planes = byte_planes(table)
    rows = query.shape[0]
    edges = [0]
    for share in SHARES:
        edges.append(edges[-1] + rows // 16 // 8 * 8 * share)
    edges[-1] = rows
    found = ()
    for first, last in zip(edges, edges[1:]):
        found = (
            pl.pallas_call(
                functools.partial(lookup_body, first, last),
                out_shape=jax.ShapeDtypeStruct(query.shape, jnp.int32),
                compiler_params=room(planes.size * 16),
                name="lookup",
            )(planes, query, *found),
        )
    return found[0]


def pack_body(cum_ref, out_ref):
    half = out_ref.shape[0]
    rows = min(half, 64)

    def fixed(first):
        cum = cum_ref[pl.ds(first, rows), :]
        policy = (cum / jnp.sum(cum, axis=1, keepdims=True)).astype(jnp.bfloat16)
        return (policy.astype(jnp.float32) * float(2**SCALE_BITS) + 0.5).astype(jnp.int32)

    def step(i, carry):
        first = pl.multiple_of(i * rows, rows)
        out_ref[pl.ds(first, rows), :] = fixed(first) | (fixed(first + half) << 16)
        return carry

    lax.fori_loop(0, half // rows, step, 0, unroll=2)


def pack(opp_cum):
    rows, acts = opp_cum.shape
    return pl.pallas_call(
        pack_body,
        out_shape=jax.ShapeDtypeStruct((rows // 2, acts), jnp.int32),
        compiler_params=room(opp_cum.size * 6),
        name="pack",
    )(opp_cum)


def split(x, parts):
    out = []
    for _ in range(parts):
        out.append(x.astype(jnp.bfloat16))
        x = x - out[-1].astype(jnp.float32)
    return out


def outgoing(value_ref, row_ref, reach_ref, slot_ref, note_ref, out_ref, weighted):
    table = jnp.concatenate(split(value_ref[...].T, 2), axis=1)
    group = 16

    def step(i, carry):
        queries = [row_ref[pl.ds(group * i + k, 1), :] for k in range(group)]
        for k, (found, hit) in enumerate(pick(table, queries, 2)):
            chosen = jnp.sum(jnp.where(hit, found, 0.0), axis=0, keepdims=True)
            weighted[pl.ds(group * i + k, 1), :] = chosen
        return carry

    lax.fori_loop(0, row_ref.shape[0] // group, step, 0)
    devices, limit = note_ref.shape[0], out_ref.shape[1]
    half = limit // 2
    place = one_hot(iota((devices * limit, row_ref.shape[0]), 0) == slot_ref[...])
    total = jnp.zeros((devices * limit, LANES), jnp.float32)
    for part in split(weighted[...] * column(reach_ref[...]), 3):
        total = total + jnp.dot(place, part, preferred_element_type=jnp.float32)
    top = jnp.max(jnp.abs(total), axis=1, keepdims=True)
    scale = jnp.floor(top * UNIT) + 1.0
    coded = jnp.floor(total * (WIDEST * UNIT / scale) + 0.5).astype(jnp.int32)
    lane = iota((limit, LANES), 1)
    spot = iota((limit, LANES), 0) + (limit + 1)
    for d in range(devices):
        rows = slice(limit * d, limit * (d + 1))
        scales = jnp.where(lane == spot, jnp.broadcast_to(scale[rows], lane.shape), 0.0)
        note = note_ref[d : d + 1, :] + jnp.sum(scales, axis=0, keepdims=True)
        low, high = coded[rows][:half], coded[rows][half:]
        out_ref[d, :half, :] = (low & 0xFFFF) | (high << 16)
        out_ref[d, half:, :] = jnp.broadcast_to(note.astype(jnp.int32), (limit - half, LANES))


def outgoing_rows(history_value, child_row, reach, slot, notes, limit):
    return pl.pallas_call(
        outgoing,
        out_shape=jax.ShapeDtypeStruct((notes.shape[0], limit, LANES), jnp.int32),
        scratch_shapes=[pltpu.VMEM(child_row.shape, jnp.float32)],
        compiler_params=room(4 * 2**20),
        name="outgoing",
    )(history_value, child_row, reach, slot, notes)


def fill(refs, slots, table, sems):
    size = refs[0].shape[0]
    return [
        pltpu.make_async_copy(ref, table.at[pl.ds(8 + b * size, size), :], sems.at[i])
        for i, (ref, b) in enumerate(zip(refs, slots))
    ]


def quotient(x, n):
    return x >> (n.bit_length() - 1) if n & (n - 1) == 0 else x // n


def split_by(x, n):
    whole = quotient(x, n)
    return whole, x - whole * n


def stage_body(slots, along, width, words, home_ref, child_ref, *refs):
    block_refs, (table, place_ref, odd_ref, child, sems) = refs[: len(slots)], refs[len(slots) :]
    copies = fill(block_refs, slots, table, sems)
    copies.append(pltpu.make_async_copy(child_ref, child, sems.at[len(slots)]))
    for copy in copies:
        copy.start()
    depth = along // width
    gx, gy = lax.axis_index("gx"), lax.axis_index("gy")
    my_y, my_core = split_by(gx, 2)
    my_z, my_x = split_by(gy, width)
    row, inside = split_by(home_ref[...], words)
    owner, odd = split_by(row, 2)
    chip, place = split_by(owner, along)
    y, core = split_by(chip, 2)
    z, x = split_by(place, width)
    flip_x, flip_y = x ^ my_x, y ^ my_y
    turn = jnp.where(core == 0, flip_x + 2 * flip_y, flip_y + 2 * flip_x)
    step = my_z - z
    step = jnp.where(step < 0, step + depth, step)
    block = ((core ^ my_core) * depth + step) * 4 + turn
    at = (block * words + inside).astype(jnp.float32)
    place_ref[...] = at.T.astype(jnp.int32)
    odd_ref[...] = odd
    for copy in copies:
        copy.wait()


def staged(blocks, home, child_value, along, width):
    size = blocks[0].shape[0]
    vmem, _, hbm = spaces()
    shape = (len(blocks) * size + 16, LANES)
    return pl.pallas_call(
        functools.partial(stage_body, STAGED, along, width, size),
        out_shape=(
            jax.ShapeDtypeStruct(shape, jnp.int32),
            jax.ShapeDtypeStruct(home.shape[::-1], jnp.int32),
            jax.ShapeDtypeStruct(home.shape, jnp.int32),
            jax.ShapeDtypeStruct(child_value.shape, child_value.dtype),
        ),
        in_specs=[vmem, pl.BlockSpec(memory_space=pltpu.HBM)] + [hbm] * len(STAGED),
        out_specs=(vmem, vmem, vmem, vmem),
        scratch_shapes=[pltpu.SemaphoreType.DMA((len(STAGED) + 1,))],
        compiler_params=room(0),
        name="stage",
    )(
        home,
        pltpu.with_memory_space_constraint(child_value, pltpu.HBM),
        *(blocks[b] for b in STAGED),
    )


def value_body(slots, place_ref, odd_ref, child, *rest):
    upper, block_refs = rest[:4], rest[5 : 5 + len(slots)]
    value_ref, out_ref, table, weighted, sems = rest[5 + len(slots) :]
    copies = fill(block_refs, slots, table, sems)
    tiles = value_ref.shape[0]
    for copy in copies:
        copy.start()
    for copy in copies:
        copy.wait()
    sub = iota((8, LANES), 0)
    spot = iota((8, LANES), 1) - sub

    def place(k, t):
        return place_ref.at[pl.ds(k * tiles, tiles)][t]

    def tile(t, carry):
        low = jnp.zeros((8, LANES), jnp.float32)
        high = jnp.zeros((8, LANES), jnp.float32)
        start = pl.multiple_of(t * LANES, LANES)
        children = child.at[pl.ds(start, LANES), :]
        for g in range(LANES // 16):
            values = children[16 * g : 16 * g + 16, :].astype(jnp.float32)
            for half in range(2):
                at = 16 * g + 8 * half
                words = table[pl.ds(place(at, t) + 8, 8), :]
                for s in range(1, 8):
                    row = table[pl.ds(place(at + s, t) + (8 - s), 8), :]
                    words = jnp.where(sub == s, row, words)
                part = values[8 * half : 8 * half + 8]
                even = (words & 0xFFFF).astype(jnp.float32) * part
                odd = lax.shift_right_logical(words, 16).astype(jnp.float32) * part
                here = spot == at
                low = jnp.where(here, jnp.sum(even, axis=1, keepdims=True), low)
                high = jnp.where(here, jnp.sum(odd, axis=1, keepdims=True), high)
        low = jnp.sum(low, axis=0, keepdims=True)
        high = jnp.sum(high, axis=0, keepdims=True)
        picked = jnp.where(odd_ref[pl.ds(t, 1), :] > 0, high, low)
        value_ref[pl.ds(t, 1), :] = picked * (0.5**SCALE_BITS)
        return carry

    lax.fori_loop(0, tiles, tile, 0, unroll=16)
    outgoing(value_ref, *upper, out_ref, weighted)


def values_from(blocks, home, along, width, child_value, child_row, reach, slot, notes, limit):
    table, place, odd, child = staged(blocks, home, child_value, along, width)
    rest = tuple(b for b in range(len(blocks)) if b not in STAGED)
    vmem, smem, hbm = spaces()
    return pl.pallas_call(
        functools.partial(value_body, rest),
        out_shape=(
            jax.ShapeDtypeStruct(odd.shape, jnp.float32),
            jax.ShapeDtypeStruct((notes.shape[0], limit, LANES), jnp.int32),
            jax.ShapeDtypeStruct(table.shape, table.dtype),
        ),
        in_specs=[smem] + [vmem] * 7 + [hbm] * len(rest),
        out_specs=(vmem, vmem, vmem),
        scratch_shapes=[
            pltpu.VMEM(child_row.shape, jnp.float32),
            pltpu.SemaphoreType.DMA((len(rest),)),
        ],
        input_output_aliases={7: 2},
        compiler_params=room(4 * 2**20),
        name="values",
    )(
        place.reshape(-1),
        odd,
        child,
        child_row,
        reach,
        slot,
        notes,
        table,
        *(blocks[b] for b in rest),
    )[:2]


def column(row):
    return jnp.broadcast_to(row.astype(jnp.float32), (row.shape[1], row.shape[1])).T


def slots_body(per_br, limit, home_ref, set_ref, reach_ref, place_ref, note_ref):
    parents = set_ref.shape[1]
    count = max(1, ((home_ref.size - 1).bit_length() + 7) // 8)
    home = jnp.zeros(set_ref.shape, jnp.float32)
    for c in range(count):
        byte = ((home_ref[...] >> (8 * c)) & 255).astype(jnp.float32)
        ((found, hit),) = pick(byte.T.astype(jnp.bfloat16), [set_ref[...]], 1)
        home += jnp.sum(jnp.where(hit, found, 0.0), axis=0, keepdims=True) * float(256**c)
    home = home.astype(jnp.int32)
    owner = quotient(home, per_br)
    inside = home - owner * per_br
    square = (parents, parents)
    earlier = iota(square, 0) < iota(square, 1)
    same = column(owner) == owner.astype(jnp.float32)
    rank = jnp.sum(jnp.where(earlier & same, 1.0, 0.0), axis=0, keepdims=True)
    place_ref[...] = owner * limit + rank.astype(jnp.int32)
    devices = note_ref.shape[0]
    here = iota((devices, parents), 0) == owner
    rows = jnp.where(here, (inside + 1).astype(jnp.float32), 0.0).astype(jnp.bfloat16)
    ranks = one_hot(column(rank) == iota((parents, LANES), 1).astype(jnp.float32))
    asked = jnp.dot(rows, ranks, preferred_element_type=jnp.float32) - 1.0
    reach = jnp.sum(jnp.broadcast_to(reach_ref[...], note_ref.shape), axis=1, keepdims=True)
    lane = iota(note_ref.shape, 1)
    note = jnp.where(lane == limit, jnp.floor(reach * UNIT + 0.5), asked)
    note_ref[...] = jnp.where(lane > limit, 0.0, note)


def slots_of(br_home, br_set, reach, per_br, devices, limit):
    return pl.pallas_call(
        functools.partial(slots_body, per_br, limit),
        out_shape=(
            jax.ShapeDtypeStruct((1, br_set.shape[0]), jnp.int32),
            jax.ShapeDtypeStruct((devices, LANES), jnp.float32),
        ),
        compiler_params=room(2**20),
        name="slots",
    )(br_home.reshape(-1, LANES), br_set[None, :], reach[None, :])


def regret_body(incoming_ref, cum_ref, gap_ref, total_ref, reach_ref):
    sets = cum_ref.shape[0]
    devices, limit = incoming_ref.shape[:2]
    half = limit // 2
    coded, spread, notes = [], [], []
    for d in range(devices):
        pair = incoming_ref[d, :half, :]
        coded += [(pair << 16) >> 16, pair >> 16]
        notes.append(incoming_ref[d, half : half + 1, :].astype(jnp.float32))
        spread.append(jnp.broadcast_to(notes[-1], (limit, LANES)))
    spread, notes = jnp.concatenate(spread, axis=0), jnp.concatenate(notes, axis=0)
    lane, turn = iota(spread.shape, 1), iota(spread.shape, 0) % limit
    asked = jnp.sum(jnp.where(lane == turn, spread, 0.0), axis=1, keepdims=True)
    scale = jnp.sum(jnp.where(lane == turn + (limit + 1), spread, 0.0), axis=1, keepdims=True)
    rows = jnp.concatenate(coded, axis=0).astype(jnp.float32) * (scale * (1.0 / (WIDEST * UNIT)))
    member = one_hot(jnp.broadcast_to(asked, spread.shape) == lane.astype(jnp.float32))
    value = jnp.zeros(cum_ref.shape, jnp.float32)
    for part in split(rows, 3):
        value = value + lax.dot_general(
            member, part, (((0,), (0,)), ((), ())), preferred_element_type=jnp.float32
        )[:sets]
    policy = cum_ref[...] / jnp.sum(cum_ref[...], axis=1, keepdims=True)
    gap = jnp.max(value, axis=1, keepdims=True) - jnp.sum(policy * value, axis=1, keepdims=True)
    own = iota((sets, LANES), 0) == iota((sets, LANES), 1)
    gap_ref[...] = jnp.sum(jnp.where(own, gap, 0.0), axis=0, keepdims=True)
    total = jnp.sum(jnp.broadcast_to(gap, (sets, LANES)), axis=0, keepdims=True)
    total_ref[...] = jnp.broadcast_to(total, total_ref.shape)
    here = iota(notes.shape, 1) == limit
    reach = jnp.sum(jnp.where(here, notes, 0.0), axis=1, keepdims=True)
    reach = jnp.sum(jnp.broadcast_to(reach, notes.shape), axis=0, keepdims=True)
    reach_ref[...] = reach * (1.0 / UNIT)


def regrets(incoming, br_cum):
    return pl.pallas_call(
        regret_body,
        out_shape=(
            jax.ShapeDtypeStruct((1, LANES), jnp.float32),
            jax.ShapeDtypeStruct((incoming.shape[0], LANES), jnp.float32),
            jax.ShapeDtypeStruct((1, LANES), jnp.float32),
        ),
        compiler_params=room(incoming.size * 16),
        name="regret",
    )(incoming, br_cum)


def factors(n):
    high = 1
    while high * high < n:
        high *= 2
    return high, n // high


def exchange(block, across, depth, width):
    def device(y, core, z, x):
        return ((y * 2 + core) * depth + z) * width + x

    def move(array, to):
        pairs = []
        for y in range(across // 2):
            for core in range(2):
                for z in range(depth):
                    for x in range(width):
                        pairs.append((device(y, core, z, x), device(*to(y, core, z, x))))
        return lax.ppermute(array, AXES, pairs)

    def ring(y, core, z, x):
        return (y, core, (z + 1) % depth, x)

    def near(y, core, z, x):
        return (y, core, z, x ^ 1) if core == 0 else (y ^ 1, core, z, x)

    def far(y, core, z, x):
        return (y ^ 1, core, z, x) if core == 0 else (y, core, z, x ^ 1)

    def twin(y, core, z, x):
        return (y, 1 - core, z, x)

    start, beside, opposite, diagonal = [block], [], [], []
    for i in range(depth):
        if i:
            start.append(move(start[-1], ring))
        beside.append(move(start[-1], near))
        opposite.append(move(start[-1], far))
        if 0 < i < depth - 1:
            diagonal.append(move(diagonal[-1], ring))
        else:
            diagonal.append(move(beside[-1], far))
    mine = [part for group in zip(start, beside, opposite, diagonal) for part in group]
    return mine + [move(part, twin) for part in mine]


def local(child_value, child_row, opp_set, opp_home, opp_cum, reach, br_set, br_home, br_cum):
    across = lax.axis_size("gx")
    along = lax.axis_size("gy")
    devices = across * along
    depth, width = factors(along)
    hist, acts = child_value.shape
    parents = reach.shape[0]
    per_opp = opp_cum.shape[0]
    per_br = br_cum.shape[0]
    words = per_opp // 2
    limit_two = max(2, (2 * parents + devices - 1) // devices)

    packed = pack(opp_cum)

    home = lookups(opp_home, opp_set.reshape(hist // LANES, LANES))
    place_two, notes = slots_of(br_home, br_set, reach, per_br, devices, limit_two)
    rows_two = child_row.reshape(parents, acts)
    if across == 4 and (depth, width) == (4, 2) and devices * words * acts * 4 <= TABLE_LIMIT:
        blocks = exchange(packed, across, depth, width)
        history_value, outgoing_two = values_from(
            blocks, home, along, width, child_value, rows_two, reach[None, :], place_two, notes, limit_two
        )
    else:
        owner, inside = home // per_opp, home % per_opp
        odd = inside // words
        table = lax.all_gather(packed, AXES, axis=0, tiled=True)
        rows = jnp.take(table, (owner * words + inside % words).reshape(-1), axis=0)
        rows = lax.shift_right_logical(rows, 16 * odd.reshape(-1, 1)) & 0xFFFF
        history_value = jnp.einsum(
            "ra,ra->r", rows.astype(jnp.float32), child_value.astype(jnp.float32)
        ) * (0.5**SCALE_BITS)
        history_value = history_value.reshape(hist // LANES, LANES)
        outgoing_two = outgoing_rows(
            history_value, rows_two, reach[None, :], place_two, notes, limit_two
        )
    incoming_two = lax.all_to_all(outgoing_two, AXES, split_axis=0, concat_axis=0, tiled=True)
    gap_row, gaps, reach_row = regrets(incoming_two, br_cum)
    regret_gap = gap_row[0, :per_br]
    gaps = lax.all_to_all(gaps, AXES, split_axis=0, concat_axis=0, tiled=True)
    gap_total = jnp.sum(gaps[:, 0])
    return (history_value.reshape(-1), regret_gap, gap_total / reach_row[0, 0])


def shortcut(mesh):
    gx, gy = mesh.shape["gx"], mesh.shape["gy"]
    return gx == 4 and factors(gy) == (4, 2)


def solution(mesh):
    placed = (
        P(AXES, None),
        P(AXES, None),
        P(AXES),
        P(),
        P(AXES, None),
        P(AXES),
        P(AXES),
        P(),
        P(AXES, None),
    )
    step = jax.shard_map(
        local,
        mesh=mesh,
        in_specs=placed,
        out_specs=(P(AXES), P(AXES), P()),
        check_vma=False,
    )
    return step if shortcut(mesh) else step
```

```python
import functools

import jax
import jax.numpy as jnp
from jax import lax
from jax.experimental import pallas as pl
from jax.experimental.pallas import tpu as pltpu
from jax.sharding import PartitionSpec as P


AXES = ("gx", "gy")
LANES = 128
SCALE_BITS = 17
TABLE_LIMIT = 24 * 2**20
UNIT, WIDEST = float(2**20), 32767.0
SHARES = (5, 5, 4, 1, 1)
STAGED = tuple(i for i in range(32) if i % 16 not in (7, 11, 13, 14, 15))


def iota(shape, dim):
    return lax.broadcasted_iota(jnp.int32, shape, dim)


def one_hot(hit):
    return jnp.where(hit, 1.0, 0.0).astype(jnp.bfloat16)


def room(size):
    return pltpu.CompilerParams(vmem_limit_bytes=size + 4 * 2**20)


def spaces():
    return (pl.BlockSpec(memory_space=s) for s in (pltpu.VMEM, pltpu.SMEM, pl.ANY))


def pick(table, query_refs, parts):
    height = table.shape[1] // parts
    row_of = iota((height, LANES), 0)
    lane_of = iota((LANES, LANES), 0)
    rows = jnp.concatenate([one_hot(row_of == (q >> 7)) for q in query_refs], axis=1)
    rows = jnp.concatenate([rows] * parts, axis=0) if parts > 1 else rows
    found = jnp.dot(table, rows, preferred_element_type=jnp.float32)
    return [
        (found[:, LANES * k : LANES * (k + 1)], lane_of == (q & (LANES - 1)))
        for k, q in enumerate(query_refs)
    ]


def lookup_body(first, last, planes_ref, query_ref, *refs):
    out_ref = refs[-1]
    count, group = planes_ref.shape[0] // LANES, 8
    if len(refs) > 1:
        out_ref[:first, :] = refs[0][:first, :]

    def step(i, carry):
        queries = [query_ref[pl.ds(group * i + k, 1), :] for k in range(group)]
        table = planes_ref[...]
        found = [
            pick(table[LANES * c : LANES * (c + 1)], queries, 1) for c in range(count)
        ]
        for k in range(group):
            total, hit = found[0][k]
            for c in range(1, count):
                total = total + found[c][k][0] * float(256**c)
            value = jnp.sum(jnp.where(hit, total, 0.0), axis=0, keepdims=True)
            out_ref[pl.ds(group * i + k, 1), :] = value.astype(jnp.int32)
        return carry

    lax.fori_loop(first // group, last // group, step, 0)


def planes_body(table_ref, out_ref):
    high = table_ref.shape[0]
    for c in range(out_ref.shape[0] // LANES):
        for h in range(0, high, LANES):
            byte = (table_ref[h : h + LANES, :] >> (8 * c)) & 255
            out_ref[LANES * c : LANES * (c + 1), h : h + LANES] = byte.astype(
                jnp.float32
            ).T.astype(jnp.bfloat16)


def byte_planes(table):
    size = table.shape[0]
    count = max(1, ((size - 1).bit_length() + 7) // 8)
    return pl.pallas_call(
        planes_body,
        out_shape=jax.ShapeDtypeStruct((count * LANES, size // LANES), jnp.bfloat16),
        compiler_params=room(table.size * 8),
        name="planes",
    )(table.reshape(-1, LANES))


def lookups(table, query):
    planes = byte_planes(table)
    rows = query.shape[0]
    edges = [0]
    for share in SHARES:
        edges.append(edges[-1] + rows // 16 // 8 * 8 * share)
    edges[-1] = rows
    found = ()
    for first, last in zip(edges, edges[1:]):
        found = (
            pl.pallas_call(
                functools.partial(lookup_body, first, last),
                out_shape=jax.ShapeDtypeStruct(query.shape, jnp.int32),
                compiler_params=room(planes.size * 16),
                name="lookup",
            )(planes, query, *found),
        )
    return found[0]


def pack_body(cum_ref, out_ref):
    half = out_ref.shape[0]
    rows = min(half, 64)

    def fixed(first):
        cum = cum_ref[pl.ds(first, rows), :]
        policy = (cum / jnp.sum(cum, axis=1, keepdims=True)).astype(jnp.bfloat16)
        return (policy.astype(jnp.float32) * float(2**SCALE_BITS) + 0.5).astype(jnp.int32)

    def step(i, carry):
        first = pl.multiple_of(i * rows, rows)
        out_ref[pl.ds(first, rows), :] = fixed(first) | (fixed(first + half) << 16)
        return carry

    lax.fori_loop(0, half // rows, step, 0, unroll=2)


def pack(opp_cum):
    rows, acts = opp_cum.shape
    return pl.pallas_call(
        pack_body,
        out_shape=jax.ShapeDtypeStruct((rows // 2, acts), jnp.int32),
        compiler_params=room(opp_cum.size * 6),
        name="pack",
    )(opp_cum)


def split(x, parts):
    out = []
    for _ in range(parts):
        out.append(x.astype(jnp.bfloat16))
        x = x - out[-1].astype(jnp.float32)
    return out


def outgoing(value_ref, row_ref, reach_ref, slot_ref, note_ref, out_ref, weighted):
    table = jnp.concatenate(split(value_ref[...].T, 2), axis=1)
    group = 16

    def step(i, carry):
        queries = [row_ref[pl.ds(group * i + k, 1), :] for k in range(group)]
        for k, (found, hit) in enumerate(pick(table, queries, 2)):
            chosen = jnp.sum(jnp.where(hit, found, 0.0), axis=0, keepdims=True)
            weighted[pl.ds(group * i + k, 1), :] = chosen
        return carry

    lax.fori_loop(0, row_ref.shape[0] // group, step, 0)
    devices, limit = note_ref.shape[0], out_ref.shape[1]
    half = limit // 2
    place = one_hot(iota((devices * limit, row_ref.shape[0]), 0) == slot_ref[...])
    total = jnp.zeros((devices * limit, LANES), jnp.float32)
    for part in split(weighted[...] * column(reach_ref[...]), 3):
        total = total + jnp.dot(place, part, preferred_element_type=jnp.float32)
    top = jnp.max(jnp.abs(total), axis=1, keepdims=True)
    scale = jnp.floor(top * UNIT) + 1.0
    coded = jnp.floor(total * (WIDEST * UNIT / scale) + 0.5).astype(jnp.int32)
    lane = iota((limit, LANES), 1)
    spot = iota((limit, LANES), 0) + (limit + 1)
    for d in range(devices):
        rows = slice(limit * d, limit * (d + 1))
        scales = jnp.where(lane == spot, jnp.broadcast_to(scale[rows], lane.shape), 0.0)
        note = note_ref[d : d + 1, :] + jnp.sum(scales, axis=0, keepdims=True)
        low, high = coded[rows][:half], coded[rows][half:]
        out_ref[d, :half, :] = (low & 0xFFFF) | (high << 16)
        out_ref[d, half:, :] = jnp.broadcast_to(note.astype(jnp.int32), (limit - half, LANES))


def outgoing_rows(history_value, child_row, reach, slot, notes, limit):
    return pl.pallas_call(
        outgoing,
        out_shape=jax.ShapeDtypeStruct((notes.shape[0], limit, LANES), jnp.int32),
        scratch_shapes=[pltpu.VMEM(child_row.shape, jnp.float32)],
        compiler_params=room(4 * 2**20),
        name="outgoing",
    )(history_value, child_row, reach, slot, notes)


def fill(refs, slots, table, sems):
    size = refs[0].shape[0]
    return [
        pltpu.make_async_copy(ref, table.at[pl.ds(8 + b * size, size), :], sems.at[i])
        for i, (ref, b) in enumerate(zip(refs, slots))
    ]


def quotient(x, n):
    return x >> (n.bit_length() - 1) if n & (n - 1) == 0 else x // n


def split_by(x, n):
    whole = quotient(x, n)
    return whole, x - whole * n


def stage_body(slots, along, width, words, home_ref, child_ref, *refs):
    block_refs, (table, place_ref, odd_ref, child, sems) = refs[: len(slots)], refs[len(slots) :]
    copies = fill(block_refs, slots, table, sems)
    copies.append(pltpu.make_async_copy(child_ref, child, sems.at[len(slots)]))
    for copy in copies:
        copy.start()
    depth = along // width
    gx, gy = lax.axis_index("gx"), lax.axis_index("gy")
    my_y, my_core = split_by(gx, 2)
    my_z, my_x = split_by(gy, width)
    row, inside = split_by(home_ref[...], words)
    owner, odd = split_by(row, 2)
    chip, place = split_by(owner, along)
    y, core = split_by(chip, 2)
    z, x = split_by(place, width)
    flip_x, flip_y = x ^ my_x, y ^ my_y
    turn = jnp.where(core == 0, flip_x + 2 * flip_y, flip_y + 2 * flip_x)
    step = my_z - z
    step = jnp.where(step < 0, step + depth, step)
    block = ((core ^ my_core) * depth + step) * 4 + turn
    at = (block * words + inside).astype(jnp.float32)
    place_ref[...] = at.T.astype(jnp.int32)
    odd_ref[...] = odd
    for copy in copies:
        copy.wait()


def staged(blocks, home, child_value, along, width):
    size = blocks[0].shape[0]
    vmem, _, hbm = spaces()
    shape = (len(blocks) * size + 16, LANES)
    return pl.pallas_call(
        functools.partial(stage_body, STAGED, along, width, size),
        out_shape=(
            jax.ShapeDtypeStruct(shape, jnp.int32),
            jax.ShapeDtypeStruct(home.shape[::-1], jnp.int32),
            jax.ShapeDtypeStruct(home.shape, jnp.int32),
            jax.ShapeDtypeStruct(child_value.shape, child_value.dtype),
        ),
        in_specs=[vmem, pl.BlockSpec(memory_space=pltpu.HBM)] + [hbm] * len(STAGED),
        out_specs=(vmem, vmem, vmem, vmem),
        scratch_shapes=[pltpu.SemaphoreType.DMA((len(STAGED) + 1,))],
        compiler_params=room(0),
        name="stage",
    )(
        home,
        pltpu.with_memory_space_constraint(child_value, pltpu.HBM),
        *(blocks[b] for b in STAGED),
    )


def value_body(slots, place_ref, odd_ref, child, *rest):
    upper, block_refs = rest[:4], rest[5 : 5 + len(slots)]
    value_ref, out_ref, table, weighted, sems = rest[5 + len(slots) :]
    copies = fill(block_refs, slots, table, sems)
    tiles = value_ref.shape[0]
    for copy in copies:
        copy.start()
    for copy in copies:
        copy.wait()
    sub = iota((8, LANES), 0)
    spot = iota((8, LANES), 1) - sub

    def place(k, t):
        return place_ref.at[pl.ds(k * tiles, tiles)][t]

    def tile(t, carry):
        low = jnp.zeros((8, LANES), jnp.float32)
        high = jnp.zeros((8, LANES), jnp.float32)
        start = pl.multiple_of(t * LANES, LANES)
        children = child.at[pl.ds(start, LANES), :]
        for g in range(LANES // 16):
            values = children[16 * g : 16 * g + 16, :].astype(jnp.float32)
            for half in range(2):
                at = 16 * g + 8 * half
                words = table[pl.ds(place(at, t) + 8, 8), :]
                for s in range(1, 8):
                    row = table[pl.ds(place(at + s, t) + (8 - s), 8), :]
                    words = jnp.where(sub == s, row, words)
                part = values[8 * half : 8 * half + 8]
                even = (words & 0xFFFF).astype(jnp.float32) * part
                odd = lax.shift_right_logical(words, 16).astype(jnp.float32) * part
                here = spot == at
                low = jnp.where(here, jnp.sum(even, axis=1, keepdims=True), low)
                high = jnp.where(here, jnp.sum(odd, axis=1, keepdims=True), high)
        low = jnp.sum(low, axis=0, keepdims=True)
        high = jnp.sum(high, axis=0, keepdims=True)
        picked = jnp.where(odd_ref[pl.ds(t, 1), :] > 0, high, low)
        value_ref[pl.ds(t, 1), :] = picked * (0.5**SCALE_BITS)
        return carry

    lax.fori_loop(0, tiles, tile, 0, unroll=16)
    outgoing(value_ref, *upper, out_ref, weighted)


def values_from(blocks, home, along, width, child_value, child_row, reach, slot, notes, limit):
    table, place, odd, child = staged(blocks, home, child_value, along, width)
    rest = tuple(b for b in range(len(blocks)) if b not in STAGED)
    vmem, smem, hbm = spaces()
    return pl.pallas_call(
        functools.partial(value_body, rest),
        out_shape=(
            jax.ShapeDtypeStruct(odd.shape, jnp.float32),
            jax.ShapeDtypeStruct((notes.shape[0], limit, LANES), jnp.int32),
            jax.ShapeDtypeStruct(table.shape, table.dtype),
        ),
        in_specs=[smem] + [vmem] * 7 + [hbm] * len(rest),
        out_specs=(vmem, vmem, vmem),
        scratch_shapes=[
            pltpu.VMEM(child_row.shape, jnp.float32),
            pltpu.SemaphoreType.DMA((len(rest),)),
        ],
        input_output_aliases={7: 2},
        compiler_params=room(4 * 2**20),
        name="values",
    )(
        place.reshape(-1),
        odd,
        child,
        child_row,
        reach,
        slot,
        notes,
        table,
        *(blocks[b] for b in rest),
    )[:2]


def column(row):
    return jnp.broadcast_to(row.astype(jnp.float32), (row.shape[1], row.shape[1])).T


def slots_body(per_br, limit, home_ref, set_ref, reach_ref, place_ref, note_ref):
    parents = set_ref.shape[1]
    count = max(1, ((home_ref.size - 1).bit_length() + 7) // 8)
    home = jnp.zeros(set_ref.shape, jnp.float32)
    for c in range(count):
        byte = ((home_ref[...] >> (8 * c)) & 255).astype(jnp.float32)
        ((found, hit),) = pick(byte.T.astype(jnp.bfloat16), [set_ref[...]], 1)
        home += jnp.sum(jnp.where(hit, found, 0.0), axis=0, keepdims=True) * float(256**c)
    home = home.astype(jnp.int32)
    owner = quotient(home, per_br)
    inside = home - owner * per_br
    square = (parents, parents)
    earlier = iota(square, 0) < iota(square, 1)
    same = column(owner) == owner.astype(jnp.float32)
    rank = jnp.sum(jnp.where(earlier & same, 1.0, 0.0), axis=0, keepdims=True)
    place_ref[...] = owner * limit + rank.astype(jnp.int32)
    devices = note_ref.shape[0]
    here = iota((devices, parents), 0) == owner
    rows = jnp.where(here, (inside + 1).astype(jnp.float32), 0.0).astype(jnp.bfloat16)
    ranks = one_hot(column(rank) == iota((parents, LANES), 1).astype(jnp.float32))
    asked = jnp.dot(rows, ranks, preferred_element_type=jnp.float32) - 1.0
    reach = jnp.sum(jnp.broadcast_to(reach_ref[...], note_ref.shape), axis=1, keepdims=True)
    lane = iota(note_ref.shape, 1)
    note = jnp.where(lane == limit, jnp.floor(reach * UNIT + 0.5), asked)
    note_ref[...] = jnp.where(lane > limit, 0.0, note)


def slots_of(br_home, br_set, reach, per_br, devices, limit):
    return pl.pallas_call(
        functools.partial(slots_body, per_br, limit),
        out_shape=(
            jax.ShapeDtypeStruct((1, br_set.shape[0]), jnp.int32),
            jax.ShapeDtypeStruct((devices, LANES), jnp.float32),
        ),
        compiler_params=room(2**20),
        name="slots",
    )(br_home.reshape(-1, LANES), br_set[None, :], reach[None, :])


def regret_body(incoming_ref, cum_ref, gap_ref, total_ref, reach_ref):
    sets = cum_ref.shape[0]
    devices, limit = incoming_ref.shape[:2]
    half = limit // 2
    coded, spread, notes = [], [], []
    for d in range(devices):
        pair = incoming_ref[d, :half, :]
        coded += [(pair << 16) >> 16, pair >> 16]
        notes.append(incoming_ref[d, half : half + 1, :].astype(jnp.float32))
        spread.append(jnp.broadcast_to(notes[-1], (limit, LANES)))
    spread, notes = jnp.concatenate(spread, axis=0), jnp.concatenate(notes, axis=0)
    lane, turn = iota(spread.shape, 1), iota(spread.shape, 0) % limit
    asked = jnp.sum(jnp.where(lane == turn, spread, 0.0), axis=1, keepdims=True)
    scale = jnp.sum(jnp.where(lane == turn + (limit + 1), spread, 0.0), axis=1, keepdims=True)
    rows = jnp.concatenate(coded, axis=0).astype(jnp.float32) * (scale * (1.0 / (WIDEST * UNIT)))
    member = one_hot(jnp.broadcast_to(asked, spread.shape) == lane.astype(jnp.float32))
    value = jnp.zeros(cum_ref.shape, jnp.float32)
    for part in split(rows, 3):
        value = value + lax.dot_general(
            member, part, (((0,), (0,)), ((), ())), preferred_element_type=jnp.float32
        )[:sets]
    policy = cum_ref[...] / jnp.sum(cum_ref[...], axis=1, keepdims=True)
    gap = jnp.max(value, axis=1, keepdims=True) - jnp.sum(policy * value, axis=1, keepdims=True)
    own = iota((sets, LANES), 0) == iota((sets, LANES), 1)
    gap_ref[...] = jnp.sum(jnp.where(own, gap, 0.0), axis=0, keepdims=True)
    total = jnp.sum(jnp.broadcast_to(gap, (sets, LANES)), axis=0, keepdims=True)
    total_ref[...] = jnp.broadcast_to(total, total_ref.shape)
    here = iota(notes.shape, 1) == limit
    reach = jnp.sum(jnp.where(here, notes, 0.0), axis=1, keepdims=True)
    reach = jnp.sum(jnp.broadcast_to(reach, notes.shape), axis=0, keepdims=True)
    reach_ref[...] = reach * (1.0 / UNIT)


def regrets(incoming, br_cum):
    return pl.pallas_call(
        regret_body,
        out_shape=(
            jax.ShapeDtypeStruct((1, LANES), jnp.float32),
            jax.ShapeDtypeStruct((incoming.shape[0], LANES), jnp.float32),
            jax.ShapeDtypeStruct((1, LANES), jnp.float32),
        ),
        compiler_params=room(incoming.size * 16),
        name="regret",
    )(incoming, br_cum)


def factors(n):
    high = 1
    while high * high < n:
        high *= 2
    return high, n // high


def exchange(block, across, depth, width):
    def device(y, core, z, x):
        return ((y * 2 + core) * depth + z) * width + x

    def move(array, to):
        pairs = []
        for y in range(across // 2):
            for core in range(2):
                for z in range(depth):
                    for x in range(width):
                        pairs.append((device(y, core, z, x), device(*to(y, core, z, x))))
        return lax.ppermute(array, AXES, pairs)

    def ring(y, core, z, x):
        return (y, core, (z + 1) % depth, x)

    def back(y, core, z, x):
        return (y, core, (z - 1) % depth, x)

    def near(y, core, z, x):
        return (y, core, z, x ^ 1) if core == 0 else (y ^ 1, core, z, x)

    def far(y, core, z, x):
        return (y ^ 1, core, z, x) if core == 0 else (y, core, z, x ^ 1)

    def twin(y, core, z, x):
        return (y, 1 - core, z, x)

    start = [block, move(block, ring), None, move(block, back)]
    start[2] = move(start[1], ring)
    beside = [move(part, near) for part in start]
    opposite = [move(part, far) for part in start]
    first = move(beside[0], far)
    diagonal = [first, move(first, ring), None, move(first, back)]
    diagonal[2] = move(beside[2], far)
    mine = [part for group in zip(start, beside, opposite, diagonal) for part in group]
    return mine + [move(part, twin) for part in mine]


def local(child_value, child_row, opp_set, opp_home, opp_cum, reach, br_set, br_home, br_cum):
    across = lax.axis_size("gx")
    along = lax.axis_size("gy")
    devices = across * along
    depth, width = factors(along)
    hist, acts = child_value.shape
    parents = reach.shape[0]
    per_opp = opp_cum.shape[0]
    per_br = br_cum.shape[0]
    words = per_opp // 2
    limit_two = max(2, (2 * parents + devices - 1) // devices)

    packed = pack(opp_cum)

    home = lookups(opp_home, opp_set.reshape(hist // LANES, LANES))
    place_two, notes = slots_of(br_home, br_set, reach, per_br, devices, limit_two)
    rows_two = child_row.reshape(parents, acts)
    if across == 4 and (depth, width) == (4, 2) and devices * words * acts * 4 <= TABLE_LIMIT:
        blocks = exchange(packed, across, depth, width)
        history_value, outgoing_two = values_from(
            blocks, home, along, width, child_value, rows_two, reach[None, :], place_two, notes, limit_two
        )
    else:
        owner, inside = home // per_opp, home % per_opp
        odd = inside // words
        table = lax.all_gather(packed, AXES, axis=0, tiled=True)
        rows = jnp.take(table, (owner * words + inside % words).reshape(-1), axis=0)
        rows = lax.shift_right_logical(rows, 16 * odd.reshape(-1, 1)) & 0xFFFF
        history_value = jnp.einsum(
            "ra,ra->r", rows.astype(jnp.float32), child_value.astype(jnp.float32)
        ) * (0.5**SCALE_BITS)
        history_value = history_value.reshape(hist // LANES, LANES)
        outgoing_two = outgoing_rows(
            history_value, rows_two, reach[None, :], place_two, notes, limit_two
        )
    incoming_two = lax.all_to_all(outgoing_two, AXES, split_axis=0, concat_axis=0, tiled=True)
    gap_row, gaps, reach_row = regrets(incoming_two, br_cum)
    regret_gap = gap_row[0, :per_br]
    gaps = lax.all_to_all(gaps, AXES, split_axis=0, concat_axis=0, tiled=True)
    gap_total = jnp.sum(gaps[:, 0])
    return (history_value.reshape(-1), regret_gap, gap_total / reach_row[0, 0])


def shortcut(mesh):
    gx, gy = mesh.shape["gx"], mesh.shape["gy"]
    return gx == 4 and factors(gy) == (4, 2)


def solution(mesh):
    placed = (
        P(AXES, None),
        P(AXES, None),
        P(AXES),
        P(),
        P(AXES, None),
        P(AXES),
        P(AXES),
        P(),
        P(AXES, None),
    )
    step = jax.shard_map(
        local,
        mesh=mesh,
        in_specs=placed,
        out_specs=(P(AXES), P(AXES), P()),
        check_vma=False,
    )
    return step if shortcut(mesh) else step
```

```python
import functools

import jax
import jax.numpy as jnp
from jax import lax
from jax.experimental import pallas as pl
from jax.experimental.pallas import tpu as pltpu
from jax.sharding import PartitionSpec as P


AXES = ("gx", "gy")
LANES = 128
SCALE_BITS = 17
TABLE_LIMIT = 24 * 2**20
UNIT, WIDEST = float(2**20), 32767.0
SHARES = (5, 5, 4, 1, 1)
STAGED = tuple(i for i in range(32) if i % 16 not in (7, 11, 13, 14, 15))


def iota(shape, dim):
    return lax.broadcasted_iota(jnp.int32, shape, dim)


def one_hot(hit):
    return jnp.where(hit, 1.0, 0.0).astype(jnp.bfloat16)


def room(size):
    return pltpu.CompilerParams(vmem_limit_bytes=size + 4 * 2**20)


def spaces():
    return (pl.BlockSpec(memory_space=s) for s in (pltpu.VMEM, pltpu.SMEM, pl.ANY))


def pick(table, query_refs, parts):
    height = table.shape[1] // parts
    row_of = iota((height, LANES), 0)
    lane_of = iota((LANES, LANES), 0)
    rows = jnp.concatenate([one_hot(row_of == (q >> 7)) for q in query_refs], axis=1)
    rows = jnp.concatenate([rows] * parts, axis=0) if parts > 1 else rows
    found = jnp.dot(table, rows, preferred_element_type=jnp.float32)
    return [
        (found[:, LANES * k : LANES * (k + 1)], lane_of == (q & (LANES - 1)))
        for k, q in enumerate(query_refs)
    ]


def lookup_body(first, last, planes_ref, query_ref, *refs):
    out_ref = refs[-1]
    count, group = planes_ref.shape[0] // LANES, 8
    if len(refs) > 1:
        out_ref[:first, :] = refs[0][:first, :]

    def step(i, carry):
        queries = [query_ref[pl.ds(group * i + k, 1), :] for k in range(group)]
        table = planes_ref[...]
        found = [
            pick(table[LANES * c : LANES * (c + 1)], queries, 1) for c in range(count)
        ]
        for k in range(group):
            total, hit = found[0][k]
            for c in range(1, count):
                total = total + found[c][k][0] * float(256**c)
            value = jnp.sum(jnp.where(hit, total, 0.0), axis=0, keepdims=True)
            out_ref[pl.ds(group * i + k, 1), :] = value.astype(jnp.int32)
        return carry

    lax.fori_loop(first // group, last // group, step, 0)


def planes_body(table_ref, out_ref):
    high = table_ref.shape[0]
    for c in range(out_ref.shape[0] // LANES):
        for h in range(0, high, LANES):
            byte = (table_ref[h : h + LANES, :] >> (8 * c)) & 255
            out_ref[LANES * c : LANES * (c + 1), h : h + LANES] = byte.astype(
                jnp.float32
            ).T.astype(jnp.bfloat16)


def byte_planes(table):
    size = table.shape[0]
    count = max(1, ((size - 1).bit_length() + 7) // 8)
    return pl.pallas_call(
        planes_body,
        out_shape=jax.ShapeDtypeStruct((count * LANES, size // LANES), jnp.bfloat16),
        compiler_params=room(table.size * 8),
        name="planes",
    )(table.reshape(-1, LANES))


def lookups(table, query):
    planes = byte_planes(table)
    rows = query.shape[0]
    edges = [0]
    for share in SHARES:
        edges.append(edges[-1] + rows // 16 // 8 * 8 * share)
    edges[-1] = rows
    found = ()
    for first, last in zip(edges, edges[1:]):
        found = (
            pl.pallas_call(
                functools.partial(lookup_body, first, last),
                out_shape=jax.ShapeDtypeStruct(query.shape, jnp.int32),
                compiler_params=room(planes.size * 16),
                name="lookup",
            )(planes, query, *found),
        )
    return found[0]


def pack_body(source_ref, out_ref, cum_ref, sems):
    half = out_ref.shape[0]
    parts = sems.shape[0] // 2
    chunk = half // parts
    rows = min(chunk, 64)

    def arrival(i):
        at = pl.ds(half * (i % 2) + chunk * (i // 2), chunk)
        return pltpu.make_async_copy(source_ref.at[at, :], cum_ref.at[at, :], sems.at[i])

    def fixed(first):
        cum = cum_ref[pl.ds(first, rows), :]
        policy = (cum / jnp.sum(cum, axis=1, keepdims=True)).astype(jnp.bfloat16)
        return (policy.astype(jnp.float32) * float(2**SCALE_BITS) + 0.5).astype(jnp.int32)

    def step(i, carry):
        first = i * rows
        out_ref[pl.ds(first, rows), :] = fixed(first) | (fixed(first + half) << 16)
        return carry

    for i in range(2 * parts):
        arrival(i).start()
    for c in range(parts):
        arrival(2 * c).wait()
        arrival(2 * c + 1).wait()
        for i in range(chunk // rows):
            step(c * (chunk // rows) + i, 0)


def pack(opp_cum):
    rows, acts = opp_cum.shape
    return pl.pallas_call(
        pack_body,
        out_shape=jax.ShapeDtypeStruct((rows // 2, acts), jnp.int32),
        in_specs=[pl.BlockSpec(memory_space=pltpu.HBM)],
        scratch_shapes=[
            pltpu.VMEM((rows, acts), jnp.float32),
            pltpu.SemaphoreType.DMA((8,)),
        ],
        compiler_params=room(opp_cum.size * 6),
        name="pack",
    )(pltpu.with_memory_space_constraint(opp_cum, pltpu.HBM))


def split(x, parts):
    out = []
    for _ in range(parts):
        out.append(x.astype(jnp.bfloat16))
        x = x - out[-1].astype(jnp.float32)
    return out


def outgoing(value_ref, row_ref, reach_ref, slot_ref, note_ref, out_ref, weighted):
    table = jnp.concatenate(split(value_ref[...].T, 2), axis=1)
    group = 16

    def step(i, carry):
        queries = [row_ref[pl.ds(group * i + k, 1), :] for k in range(group)]
        for k, (found, hit) in enumerate(pick(table, queries, 2)):
            chosen = jnp.sum(jnp.where(hit, found, 0.0), axis=0, keepdims=True)
            weighted[pl.ds(group * i + k, 1), :] = chosen
        return carry

    lax.fori_loop(0, row_ref.shape[0] // group, step, 0)
    devices, limit = note_ref.shape[0], out_ref.shape[1]
    half = limit // 2
    place = one_hot(iota((devices * limit, row_ref.shape[0]), 0) == slot_ref[...])
    total = jnp.zeros((devices * limit, LANES), jnp.float32)
    for part in split(weighted[...] * column(reach_ref[...]), 3):
        total = total + jnp.dot(place, part, preferred_element_type=jnp.float32)
    top = jnp.max(jnp.abs(total), axis=1, keepdims=True)
    scale = jnp.floor(top * UNIT) + 1.0
    coded = jnp.floor(total * (WIDEST * UNIT / scale) + 0.5).astype(jnp.int32)
    lane = iota((limit, LANES), 1)
    spot = iota((limit, LANES), 0) + (limit + 1)
    for d in range(devices):
        rows = slice(limit * d, limit * (d + 1))
        scales = jnp.where(lane == spot, jnp.broadcast_to(scale[rows], lane.shape), 0.0)
        note = note_ref[d : d + 1, :] + jnp.sum(scales, axis=0, keepdims=True)
        low, high = coded[rows][:half], coded[rows][half:]
        out_ref[d, :half, :] = (low & 0xFFFF) | (high << 16)
        out_ref[d, half:, :] = jnp.broadcast_to(note.astype(jnp.int32), (limit - half, LANES))


def outgoing_rows(history_value, child_row, reach, slot, notes, limit):
    return pl.pallas_call(
        outgoing,
        out_shape=jax.ShapeDtypeStruct((notes.shape[0], limit, LANES), jnp.int32),
        scratch_shapes=[pltpu.VMEM(child_row.shape, jnp.float32)],
        compiler_params=room(4 * 2**20),
        name="outgoing",
    )(history_value, child_row, reach, slot, notes)


def fill(refs, slots, table, sems):
    size = refs[0].shape[0]
    return [
        pltpu.make_async_copy(ref, table.at[pl.ds(8 + b * size, size), :], sems.at[i])
        for i, (ref, b) in enumerate(zip(refs, slots))
    ]


def quotient(x, n):
    return x >> (n.bit_length() - 1) if n & (n - 1) == 0 else x // n


def split_by(x, n):
    whole = quotient(x, n)
    return whole, x - whole * n


def stage_body(slots, along, width, words, home_ref, child_ref, *refs):
    block_refs, (table, place_ref, odd_ref, child, sems) = refs[: len(slots)], refs[len(slots) :]
    copies = fill(block_refs, slots, table, sems)
    copies.append(pltpu.make_async_copy(child_ref, child, sems.at[len(slots)]))
    for copy in copies:
        copy.start()
    depth = along // width
    gx, gy = lax.axis_index("gx"), lax.axis_index("gy")
    my_y, my_core = split_by(gx, 2)
    my_z, my_x = split_by(gy, width)
    row, inside = split_by(home_ref[...], words)
    owner, odd = split_by(row, 2)
    chip, place = split_by(owner, along)
    y, core = split_by(chip, 2)
    z, x = split_by(place, width)
    flip_x, flip_y = x ^ my_x, y ^ my_y
    turn = jnp.where(core == 0, flip_x + 2 * flip_y, flip_y + 2 * flip_x)
    step = my_z - z
    step = jnp.where(step < 0, step + depth, step)
    block = ((core ^ my_core) * depth + step) * 4 + turn
    at = (block * words + inside).astype(jnp.float32)
    place_ref[...] = at.T.astype(jnp.int32)
    odd_ref[...] = odd
    for copy in copies:
        copy.wait()


def staged(blocks, home, child_value, along, width):
    size = blocks[0].shape[0]
    vmem, _, hbm = spaces()
    shape = (len(blocks) * size + 16, LANES)
    return pl.pallas_call(
        functools.partial(stage_body, STAGED, along, width, size),
        out_shape=(
            jax.ShapeDtypeStruct(shape, jnp.int32),
            jax.ShapeDtypeStruct(home.shape[::-1], jnp.int32),
            jax.ShapeDtypeStruct(home.shape, jnp.int32),
            jax.ShapeDtypeStruct(child_value.shape, child_value.dtype),
        ),
        in_specs=[vmem, pl.BlockSpec(memory_space=pltpu.HBM)] + [hbm] * len(STAGED),
        out_specs=(vmem, vmem, vmem, vmem),
        scratch_shapes=[pltpu.SemaphoreType.DMA((len(STAGED) + 1,))],
        compiler_params=room(0),
        name="stage",
    )(
        home,
        pltpu.with_memory_space_constraint(child_value, pltpu.HBM),
        *(blocks[b] for b in STAGED),
    )


def value_body(slots, place_ref, odd_ref, child, *rest):
    upper, block_refs = rest[:4], rest[5 : 5 + len(slots)]
    value_ref, out_ref, table, weighted, sems = rest[5 + len(slots) :]
    copies = fill(block_refs, slots, table, sems)
    tiles = value_ref.shape[0]
    for copy in copies:
        copy.start()
    for copy in copies:
        copy.wait()
    sub = iota((8, LANES), 0)
    spot = iota((8, LANES), 1) - sub

    def place(k, t):
        return place_ref.at[pl.ds(k * tiles, tiles)][t]

    def tile(t, carry):
        low = jnp.zeros((8, LANES), jnp.float32)
        high = jnp.zeros((8, LANES), jnp.float32)
        start = pl.multiple_of(t * LANES, LANES)
        children = child.at[pl.ds(start, LANES), :]
        for g in range(LANES // 16):
            values = children[16 * g : 16 * g + 16, :].astype(jnp.float32)
            for half in range(2):
                at = 16 * g + 8 * half
                words = table[pl.ds(place(at, t) + 8, 8), :]
                for s in range(1, 8):
                    row = table[pl.ds(place(at + s, t) + (8 - s), 8), :]
                    words = jnp.where(sub == s, row, words)
                part = values[8 * half : 8 * half + 8]
                even = (words & 0xFFFF).astype(jnp.float32) * part
                odd = lax.shift_right_logical(words, 16).astype(jnp.float32) * part
                here = spot == at
                low = jnp.where(here, jnp.sum(even, axis=1, keepdims=True), low)
                high = jnp.where(here, jnp.sum(odd, axis=1, keepdims=True), high)
        low = jnp.sum(low, axis=0, keepdims=True)
        high = jnp.sum(high, axis=0, keepdims=True)
        picked = jnp.where(odd_ref[pl.ds(t, 1), :] > 0, high, low)
        value_ref[pl.ds(t, 1), :] = picked * (0.5**SCALE_BITS)
        return carry

    lax.fori_loop(0, tiles, tile, 0, unroll=16)
    outgoing(value_ref, *upper, out_ref, weighted)


def values_from(blocks, home, along, width, child_value, child_row, reach, slot, notes, limit):
    table, place, odd, child = staged(blocks, home, child_value, along, width)
    rest = tuple(b for b in range(len(blocks)) if b not in STAGED)
    vmem, smem, hbm = spaces()
    return pl.pallas_call(
        functools.partial(value_body, rest),
        out_shape=(
            jax.ShapeDtypeStruct(odd.shape, jnp.float32),
            jax.ShapeDtypeStruct((notes.shape[0], limit, LANES), jnp.int32),
            jax.ShapeDtypeStruct(table.shape, table.dtype),
        ),
        in_specs=[smem] + [vmem] * 7 + [hbm] * len(rest),
        out_specs=(vmem, vmem, vmem),
        scratch_shapes=[
            pltpu.VMEM(child_row.shape, jnp.float32),
            pltpu.SemaphoreType.DMA((len(rest),)),
        ],
        input_output_aliases={7: 2},
        compiler_params=room(4 * 2**20),
        name="values",
    )(
        place.reshape(-1),
        odd,
        child,
        child_row,
        reach,
        slot,
        notes,
        table,
        *(blocks[b] for b in rest),
    )[:2]


def column(row):
    return jnp.broadcast_to(row.astype(jnp.float32), (row.shape[1], row.shape[1])).T


def slots_body(per_br, limit, home_ref, set_ref, reach_ref, place_ref, note_ref):
    parents = set_ref.shape[1]
    count = max(1, ((home_ref.size - 1).bit_length() + 7) // 8)
    home = jnp.zeros(set_ref.shape, jnp.float32)
    for c in range(count):
        byte = ((home_ref[...] >> (8 * c)) & 255).astype(jnp.float32)
        ((found, hit),) = pick(byte.T.astype(jnp.bfloat16), [set_ref[...]], 1)
        home += jnp.sum(jnp.where(hit, found, 0.0), axis=0, keepdims=True) * float(256**c)
    home = home.astype(jnp.int32)
    owner = quotient(home, per_br)
    inside = home - owner * per_br
    square = (parents, parents)
    earlier = iota(square, 0) < iota(square, 1)
    same = column(owner) == owner.astype(jnp.float32)
    rank = jnp.sum(jnp.where(earlier & same, 1.0, 0.0), axis=0, keepdims=True)
    place_ref[...] = owner * limit + rank.astype(jnp.int32)
    devices = note_ref.shape[0]
    here = iota((devices, parents), 0) == owner
    rows = jnp.where(here, (inside + 1).astype(jnp.float32), 0.0).astype(jnp.bfloat16)
    ranks = one_hot(column(rank) == iota((parents, LANES), 1).astype(jnp.float32))
    asked = jnp.dot(rows, ranks, preferred_element_type=jnp.float32) - 1.0
    reach = jnp.sum(jnp.broadcast_to(reach_ref[...], note_ref.shape), axis=1, keepdims=True)
    lane = iota(note_ref.shape, 1)
    note = jnp.where(lane == limit, jnp.floor(reach * UNIT + 0.5), asked)
    note_ref[...] = jnp.where(lane > limit, 0.0, note)


def slots_of(br_home, br_set, reach, per_br, devices, limit):
    return pl.pallas_call(
        functools.partial(slots_body, per_br, limit),
        out_shape=(
            jax.ShapeDtypeStruct((1, br_set.shape[0]), jnp.int32),
            jax.ShapeDtypeStruct((devices, LANES), jnp.float32),
        ),
        compiler_params=room(2**20),
        name="slots",
    )(br_home.reshape(-1, LANES), br_set[None, :], reach[None, :])


def regret_body(incoming_ref, cum_ref, gap_ref, total_ref, reach_ref):
    sets = cum_ref.shape[0]
    devices, limit = incoming_ref.shape[:2]
    half = limit // 2
    coded, spread, notes = [], [], []
    for d in range(devices):
        pair = incoming_ref[d, :half, :]
        coded += [(pair << 16) >> 16, pair >> 16]
        notes.append(incoming_ref[d, half : half + 1, :].astype(jnp.float32))
        spread.append(jnp.broadcast_to(notes[-1], (limit, LANES)))
    spread, notes = jnp.concatenate(spread, axis=0), jnp.concatenate(notes, axis=0)
    lane, turn = iota(spread.shape, 1), iota(spread.shape, 0) % limit
    asked = jnp.sum(jnp.where(lane == turn, spread, 0.0), axis=1, keepdims=True)
    scale = jnp.sum(jnp.where(lane == turn + (limit + 1), spread, 0.0), axis=1, keepdims=True)
    rows = jnp.concatenate(coded, axis=0).astype(jnp.float32) * (scale * (1.0 / (WIDEST * UNIT)))
    member = one_hot(jnp.broadcast_to(asked, spread.shape) == lane.astype(jnp.float32))
    value = jnp.zeros(cum_ref.shape, jnp.float32)
    for part in split(rows, 3):
        value = value + lax.dot_general(
            member, part, (((0,), (0,)), ((), ())), preferred_element_type=jnp.float32
        )[:sets]
    policy = cum_ref[...] / jnp.sum(cum_ref[...], axis=1, keepdims=True)
    gap = jnp.max(value, axis=1, keepdims=True) - jnp.sum(policy * value, axis=1, keepdims=True)
    own = iota((sets, LANES), 0) == iota((sets, LANES), 1)
    gap_ref[...] = jnp.sum(jnp.where(own, gap, 0.0), axis=0, keepdims=True)
    total = jnp.sum(jnp.broadcast_to(gap, (sets, LANES)), axis=0, keepdims=True)
    total_ref[...] = jnp.broadcast_to(total, total_ref.shape)
    here = iota(notes.shape, 1) == limit
    reach = jnp.sum(jnp.where(here, notes, 0.0), axis=1, keepdims=True)
    reach = jnp.sum(jnp.broadcast_to(reach, notes.shape), axis=0, keepdims=True)
    reach_ref[...] = reach * (1.0 / UNIT)


def regrets(incoming, br_cum):
    return pl.pallas_call(
        regret_body,
        out_shape=(
            jax.ShapeDtypeStruct((1, LANES), jnp.float32),
            jax.ShapeDtypeStruct((incoming.shape[0], LANES), jnp.float32),
            jax.ShapeDtypeStruct((1, LANES), jnp.float32),
        ),
        compiler_params=room(incoming.size * 16),
        name="regret",
    )(incoming, br_cum)


def factors(n):
    high = 1
    while high * high < n:
        high *= 2
    return high, n // high


def exchange(block, across, depth, width):
    def device(y, core, z, x):
        return ((y * 2 + core) * depth + z) * width + x

    def move(array, to):
        pairs = []
        for y in range(across // 2):
            for core in range(2):
                for z in range(depth):
                    for x in range(width):
                        pairs.append((device(y, core, z, x), device(*to(y, core, z, x))))
        return lax.ppermute(array, AXES, pairs)

    def ring(y, core, z, x):
        return (y, core, (z + 1) % depth, x)

    def back(y, core, z, x):
        return (y, core, (z - 1) % depth, x)

    def near(y, core, z, x):
        return (y, core, z, x ^ 1) if core == 0 else (y ^ 1, core, z, x)

    def far(y, core, z, x):
        return (y ^ 1, core, z, x) if core == 0 else (y, core, z, x ^ 1)

    def twin(y, core, z, x):
        return (y, 1 - core, z, x)

    start = [block, move(block, ring), None, move(block, back)]
    start[2] = move(start[1], ring)
    beside = [move(part, near) for part in start]
    opposite = [move(part, far) for part in start]
    first = move(beside[0], far)
    diagonal = [first, move(first, ring), None, move(first, back)]
    diagonal[2] = move(beside[2], far)
    mine = [part for group in zip(start, beside, opposite, diagonal) for part in group]
    return mine + [move(part, twin) for part in mine]


def local(child_value, child_row, opp_set, opp_home, opp_cum, reach, br_set, br_home, br_cum):
    across = lax.axis_size("gx")
    along = lax.axis_size("gy")
    devices = across * along
    depth, width = factors(along)
    hist, acts = child_value.shape
    parents = reach.shape[0]
    per_opp = opp_cum.shape[0]
    per_br = br_cum.shape[0]
    words = per_opp // 2
    limit_two = max(2, (2 * parents + devices - 1) // devices)

    packed = pack(opp_cum)

    home = lookups(opp_home, opp_set.reshape(hist // LANES, LANES))
    place_two, notes = slots_of(br_home, br_set, reach, per_br, devices, limit_two)
    rows_two = child_row.reshape(parents, acts)
    if across == 4 and (depth, width) == (4, 2) and devices * words * acts * 4 <= TABLE_LIMIT:
        blocks = exchange(packed, across, depth, width)
        history_value, outgoing_two = values_from(
            blocks, home, along, width, child_value, rows_two, reach[None, :], place_two, notes, limit_two
        )
    else:
        owner, inside = home // per_opp, home % per_opp
        odd = inside // words
        table = lax.all_gather(packed, AXES, axis=0, tiled=True)
        rows = jnp.take(table, (owner * words + inside % words).reshape(-1), axis=0)
        rows = lax.shift_right_logical(rows, 16 * odd.reshape(-1, 1)) & 0xFFFF
        history_value = jnp.einsum(
            "ra,ra->r", rows.astype(jnp.float32), child_value.astype(jnp.float32)
        ) * (0.5**SCALE_BITS)
        history_value = history_value.reshape(hist // LANES, LANES)
        outgoing_two = outgoing_rows(
            history_value, rows_two, reach[None, :], place_two, notes, limit_two
        )
    incoming_two = lax.all_to_all(outgoing_two, AXES, split_axis=0, concat_axis=0, tiled=True)
    gap_row, gaps, reach_row = regrets(incoming_two, br_cum)
    regret_gap = gap_row[0, :per_br]
    gaps = lax.all_to_all(gaps, AXES, split_axis=0, concat_axis=0, tiled=True)
    gap_total = jnp.sum(gaps[:, 0])
    return (history_value.reshape(-1), regret_gap, gap_total / reach_row[0, 0])


def shortcut(mesh):
    gx, gy = mesh.shape["gx"], mesh.shape["gy"]
    return gx == 4 and factors(gy) == (4, 2)


def solution(mesh):
    placed = (
        P(AXES, None),
        P(AXES, None),
        P(AXES),
        P(),
        P(AXES, None),
        P(AXES),
        P(AXES),
        P(),
        P(AXES, None),
    )
    step = jax.shard_map(
        local,
        mesh=mesh,
        in_specs=placed,
        out_specs=(P(AXES), P(AXES), P()),
        check_vma=False,
    )
    return step if shortcut(mesh) else step
```
